512 devices in a mesh: groups: 2 (over y), tm: 128 (over z, x), space: 2 (over core).
Axes of the slice: x: 4, y: 2, z: 32, core: 2. Of those that a mesh axis runs over, the one named last changes fastest.
The devices are a block of a 4x8x32 slice.
Arguments:
- iterate: float32 [256, 16, 16, 128], P(('groups', 'tm'), 'space'), parts along dimension 0, may hold values from -0.7 to 1.3
- source: float32 [256, 16, 16, 128], P(('groups', 'tm'), 'space'), parts along dimension 0, may hold values from -6 to 6
- diffusivity: float32 [32, 16, 128], P(('groups', 'space')), parts along dimension 0, may hold values from 0.1 to 1
Outputs:
- new_iterate: float32 [256, 16, 16, 128], P(('groups', 'tm'), 'space'), parts along dimension 0
- new_residual: float32 [256, 16, 16, 128], P(('groups', 'tm'), 'space'), parts along dimension 0
The draws below stay inside these ranges and needn't reach their ends.
There are 2 independent parts, one for each index of `groups`. The reference program is written for one: setup_inputs(seed, part) draws one part's arguments, and reference() takes and returns one part's arrays. A program takes and returns all parts, laid end to end along the dimension named above; each array names one. Nothing has to cross between parts.
All inputs are finite; a program needn't handle non-finite values.
Results may differ from the reference program's by a relative error of at most 0.0019.
Values sent between devices are 32-bit elements; how exact they have to be, the bound alone decides.
No kernel may reach another device: no remote copies, remote signals or barrier semaphores. Data moves between devices by JAX's collectives and lax.ppermute only.
A program may use at most 64 MiB of HBM per device.

```python
import math
import jax
import jax.numpy as jnp
from jax import lax

NX = 128
NY = 16
SWEEPS = 6
NT = 128
NZ = 16


def draw_iterate(key, part):
    shape = (NT, NZ, NY, NX)
    values = 0.3 + 0.25 * jax.random.normal(key, shape, jnp.float32)
    return jnp.clip(values, -0.7, 1.3)


def block_scale(rng, shape, split, low, high):
    level = 1.0
    for dim, parts in split:
        draws = jax.random.uniform(jax.random.fold_in(jax.random.fold_in(rng, 6), dim), (parts,), jnp.float32, low / len(split), high / len(split))
        level = level * jnp.repeat(jnp.exp(draws), shape[dim] // parts).reshape((-1,) + (1,) * (len(shape) - 1 - dim))
    return level


def gaussian(key, dims, spread, most, shards=(), held_as=jnp.bfloat16):
    values = jax.random.normal(key, dims, jnp.float32) * spread
    if len(shards) > 0:
        values = block_scale(key, dims, shards, -0.22, 0.18) * values
    return jnp.clip(values, min=-most, max=most).astype(held_as)


def setup_inputs(seed: int = 0, part: int = 0) -> dict:
    arg_keys = jax.random.split(jax.random.key(seed), 4)
    part_keys = jax.random.split(jax.random.fold_in(arg_keys[3], part), 4)
    return {
        "iterate": draw_iterate(jax.random.fold_in(jax.random.fold_in(arg_keys[3], part), 71), part),
        "source": gaussian(part_keys[1], (NT, NZ, NY, NX), 1.0, 6.0, ((0, 128), (1, 2)), jnp.float32),
        "diffusivity": jnp.clip(jnp.exp(math.log(1.0) - 2.3025851 * jax.random.uniform(part_keys[2], (NZ, NY, NX), jnp.float32) ** block_scale(part_keys[2], (NZ, NY, NX), ((0, 2),), -0.2, 0.2)), 0.1, 1.0),
    }


frac_order = 0.3
step_length = 0.01
gamma_factor = 0.9086387328532904


def history_weights(lags):
    scale = 1.0 / (step_length ** frac_order * gamma_factor)
    power = 1.0 - frac_order
    safe = jnp.maximum(lags, 0.0)
    upper = (safe + 1.0) ** power - safe ** power
    lower = jnp.where(safe >= 1.0, safe ** power - jnp.maximum(safe - 1.0, 0.0) ** power, 0.0)
    return jnp.where(lags >= 0.0, (upper - lower) * scale, 0.0)


def circulant_spectrum(freqs, total):
    lags = jnp.arange(total, dtype=jnp.int32)
    first = jnp.where(lags < total // 2, history_weights(lags.astype(jnp.float32)), 0.0)
    phase = ((freqs[:, None] * lags[None, :]) % total).astype(jnp.float32) * (2.0 * math.pi / total)
    real_part = jnp.sum(first[None, :] * jnp.cos(phase), axis=1)
    imag_part = -jnp.sum(first[None, :] * jnp.sin(phase), axis=1)
    return real_part, imag_part


def fourier_tables(total):
    index = jnp.arange(total, dtype=jnp.int32)
    phase = ((index[:, None] * index[None, :]) % total).astype(jnp.float32) * (2.0 * math.pi / total)
    return jnp.cos(phase), jnp.sin(phase)


def neighbour_sum(padded):
    inner = padded[..., 1:-1, :, :]
    result = padded[..., 2:, :, :] + padded[..., :-2, :, :]
    along_y = jnp.pad(inner, [(0, 0)] * (inner.ndim - 2) + [(1, 1), (0, 0)])
    result = result + along_y[..., 2:, :] + along_y[..., :-2, :]
    along_x = jnp.pad(inner, [(0, 0)] * (inner.ndim - 1) + [(1, 1)])
    return result + along_x[..., 2:] + along_x[..., :-2]


def jacobi_step(spec_re, spec_im, sol_re, sol_im, stiff_re, stiff_im, lam_re, lam_im, inv_re, inv_im):
    res_re = spec_re - (lam_re * sol_re - lam_im * sol_im) - stiff_re
    res_im = spec_im - (lam_re * sol_im + lam_im * sol_re) - stiff_im
    return sol_re + (res_re * inv_re - res_im * inv_im), sol_im + (res_re * inv_im + res_im * inv_re)


def stiffness(field, diffusivity):
    padded = jnp.pad(field, ((0, 0), (1, 1), (0, 0), (0, 0)))
    return diffusivity * (6.0 * field - neighbour_sum(padded))


def apply_time(matrix, field):
    steps = field.shape[0]
    flat = field.reshape(steps, -1)
    return jnp.dot(matrix, flat, precision=lax.Precision.HIGHEST).reshape(field.shape)


def reference(iterate, source, diffusivity):
    total = iterate.shape[0]
    times = jnp.arange(total, dtype=jnp.int32)
    toeplitz = history_weights((times[:, None] - times[None, :]).astype(jnp.float32))
    stiff_iter = stiffness(iterate, diffusivity)
    residual = source - apply_time(toeplitz, iterate) - stiff_iter
    cos_table, sin_table = fourier_tables(total)
    spec_re = apply_time(cos_table, residual)
    spec_im = -apply_time(sin_table, residual)
    lam_re, lam_im = circulant_spectrum(times, total)
    lam_re = lam_re[:, None, None, None]
    lam_im = lam_im[:, None, None, None]
    diag_re = lam_re + 6.0 * diffusivity
    denom = diag_re * diag_re + lam_im * lam_im
    inv_re = diag_re / denom
    inv_im = -lam_im / denom
    sol_re = spec_re * inv_re - spec_im * inv_im
    sol_im = spec_re * inv_im + spec_im * inv_re
    for sweep in range(SWEEPS - 1):
        stiff_re = stiffness(sol_re, diffusivity)
        stiff_im = stiffness(sol_im, diffusivity)
        sol_re, sol_im = jacobi_step(spec_re, spec_im, sol_re, sol_im, stiff_re, stiff_im, lam_re, lam_im, inv_re, inv_im)
    stiff_re = stiffness(sol_re, diffusivity)
    stiff_im = stiffness(sol_im, diffusivity)
    correction = (apply_time(cos_table, sol_re) - apply_time(sin_table, sol_im)) / total
    stiff_time = (apply_time(cos_table, stiff_re) - apply_time(sin_table, stiff_im)) / total
    image = apply_time(toeplitz, correction) + stiff_time
    step = jnp.sum(residual * image) / jnp.sum(image * image)
    return iterate + step * correction, residual - step * image
```

```python
import math

import jax
import jax.numpy as jnp
import numpy as np
from jax import lax
from jax.experimental import pallas as pl
from jax.experimental.pallas import tpu as pltpu
from jax.sharding import Mesh
from jax.sharding import PartitionSpec as P

SWEEPS = 6
TM = ("tm_0", "tm_1")
CHIPS = "tm_0"
ROW = ("tm_1", "space")
GROUPS_TM = ("groups", "tm_0", "tm_1")

frac_order = 0.3
step_length = 0.01
gamma_factor = 0.9086387328532904


def history_weights(count):
    k = np.arange(count + 1, dtype=np.float64) ** (1.0 - frac_order)
    b = k[1:] - k[:-1]
    d = np.concatenate([[1.0], b[1:] - b[:-1]])
    return d / (step_length**frac_order * gamma_factor)


def tables(total, owners):
    half = total // 2
    here = half // owners
    n = np.arange(total)
    d = history_weights(total)
    lag = n[:, None] - n[None, :]
    hist = np.where(lag >= 0, d[np.maximum(lag, 0)], 0.0)
    first = np.where(n < half, d, 0.0)
    angle = 2.0 * math.pi * ((n[:, None] * n[None, :]) % total) / total
    lam = (first[None, :] * np.exp(-1j * angle)).sum(1)
    fwd = np.zeros((owners, 2, here, total))
    inv = np.zeros((total, owners, 2, here))
    lams = np.zeros((owners, 3, here))
    for q in range(owners):
        for j in range(here):
            k = q * here + j
            if k == 0:
                fwd[q, 0, j] = 1.0
                fwd[q, 1, j] = np.cos(angle[half])
                inv[:, q, 0, j] = 1.0 / total
                inv[:, q, 1, j] = np.cos(angle[half]) / total
                lams[q, :, j] = lam[0].real, lam[half].real, 0.0
            else:
                fwd[q, 0, j] = np.cos(angle[k])
                fwd[q, 1, j] = -np.sin(angle[k])
                inv[:, q, 0, j] = 2.0 * np.cos(angle[k]) / total
                inv[:, q, 1, j] = -2.0 * np.sin(angle[k]) / total
                lams[q, :, j] = lam[k].real, lam[k].real, lam[k].imag
    fwd = fwd.reshape(total, total)
    first_mat = np.zeros((2, total, total, 2))
    first_mat[0, :, :, 0] = hist
    first_mat[1, :, :, 0] = -fwd @ hist
    first_mat[1, :, :, 1] = fwd
    flat = inv.reshape(total, total)
    second_mat = np.zeros((total, 2, owners, 2, 2 * here))
    second_mat[:, 0, :, 0] = flat.reshape(total, owners, 2 * here)
    second_mat[:, 1, :, 0] = (hist @ flat).reshape(total, owners, 2 * here)
    second_mat[:, 1, :, 1] = flat.reshape(total, owners, 2 * here)
    f32 = np.float32
    return (
        first_mat.reshape(2 * total, 2 * total).astype(f32),
        second_mat.reshape(2 * total, 2 * total).astype(f32),
        lams.astype(f32),
    )


def neighbour_sum(padded):
    inner = padded[..., 1:-1, :, :]
    result = padded[..., 2:, :, :] + padded[..., :-2, :, :]
    along_y = jnp.pad(inner, [(0, 0)] * (inner.ndim - 2) + [(1, 1), (0, 0)])
    result = result + along_y[..., 2:, :] + along_y[..., :-2, :]
    along_x = jnp.pad(inner, [(0, 0)] * (inner.ndim - 1) + [(1, 1)])
    return result + along_x[..., 2:] + along_x[..., :-2]


def make_sweeps(own, depth, here, lanes, ny):
    cols = own + 2 * depth

    def kernel(*refs):
        pieces, kap, lam, out, start, gain, ping, pong = refs[:-7], *refs[-7:]
        flat = [(ref, c) for ref in pieces for c in range(ref.shape[0])]
        lane = lax.broadcasted_iota(jnp.int32, (here, lanes), 1)
        y = lane % ny
        y_first, y_last = y == 0, y == ny - 1
        z_first, z_last = lane < ny, lane >= lanes - ny
        lam_a, lam_b, lam_i = lam[0], lam[1], lam[2]
        for c in range(cols):
            ref, at = flat[c]
            for h in range(2):
                k = jnp.broadcast_to(kap[2 * c + h : 2 * c + h + 1, :], (here, lanes))
                diag_a = lam_a + 6.0 * k
                diag_b = lam_b + 6.0 * k
                over_a = 1.0 / (diag_a * diag_a + lam_i * lam_i)
                over_b = 1.0 / (diag_b * diag_b + lam_i * lam_i)
                g_a = diag_a * over_a
                g_b = diag_b * over_b
                g_i = -lam_i * over_a
                re = ref[at, h, 0:here, :]
                im = ref[at, h, here : 2 * here, :]
                s_re = g_a * re - g_i * im
                s_im = g_b * im + g_i * re
                start[c, h, 0] = s_re
                start[c, h, 1] = s_im
                ping[c, h, 0] = s_re
                ping[c, h, 1] = s_im
                gain[c, h, 0] = g_a * k
                gain[c, h, 1] = g_b * k
                gain[c, h, 2] = g_i * k

        def around(buf, c, part):
            a, b = buf[c, 0, part], buf[c, 1, part]
            down_a, down_b = pltpu.roll(a, ny, 1), pltpu.roll(b, ny, 1)
            up_a, up_b = pltpu.roll(a, lanes - ny, 1), pltpu.roll(b, lanes - ny, 1)

            def along_y(v):
                return jnp.where(y_first, 0.0, pltpu.roll(v, 1, 1)) + jnp.where(
                    y_last, 0.0, pltpu.roll(v, lanes - 1, 1)
                )

            na = jnp.where(z_first, 0.0, down_a) + jnp.where(z_last, up_b, up_a) + along_y(a)
            nb = jnp.where(z_first, down_a, down_b) + jnp.where(z_last, 0.0, up_b) + along_y(b)
            na = na + buf[c - 1, 0, part] + buf[c + 1, 0, part]
            nb = nb + buf[c - 1, 1, part] + buf[c + 1, 1, part]
            return na, nb

        now, then = ping, pong
        for sweep in range(1, SWEEPS):
            for c in range(sweep, cols - sweep):
                n_re, n_im = around(now, c, 0), around(now, c, 1)
                for h in range(2):
                    h_a, h_b, h_i = gain[c, h, 0], gain[c, h, 1], gain[c, h, 2]
                    then[c, h, 0] = start[c, h, 0] + (h_a * n_re[h] - h_i * n_im[h])
                    then[c, h, 1] = start[c, h, 1] + (h_b * n_im[h] + h_i * n_re[h])
            now, then = then, now
        for c in range(depth, depth + own):
            for part in range(2):
                n = around(now, c, part)
                for h in range(2):
                    sol = now[c, h, part]
                    k = jnp.broadcast_to(kap[2 * c + h : 2 * c + h + 1, :], (here, lanes))
                    row = 2 * (c - depth) + h
                    out[row, 0, here * part : here * (part + 1), :] = sol
                    out[row, 1, here * part : here * (part + 1), :] = k * (6.0 * sol - n[h])

    field = (cols, 2, 2, here, lanes)
    return pl.pallas_call(
        kernel,
        out_shape=jax.ShapeDtypeStruct((2 * own, 2, 2 * here, lanes), jnp.float32),
        in_specs=[pl.BlockSpec(memory_space=pltpu.VMEM)] * 7,
        out_specs=pl.BlockSpec(memory_space=pltpu.VMEM),
        scratch_shapes=[
            pltpu.VMEM(field, jnp.float32),
            pltpu.VMEM((cols, 2, 3, here, lanes), jnp.float32),
            pltpu.VMEM(field, jnp.float32),
            pltpu.VMEM(field, jnp.float32),
        ],
        name="sweeps",
    )


def on_device(iterate, source, diffusivity):
    _, nz, ny, nx = iterate.shape
    lanes = nz * ny
    chips, own = lax.axis_size(CHIPS), lax.axis_size("tm_1")
    cores = lax.axis_size("space")
    total = chips * own
    owners = own * cores
    here = total // 2 // owners
    depth = SWEEPS
    first_mat, second_mat, lams = tables(total, owners)
    core = lax.axis_index("space")
    chip = lax.axis_index(CHIPS)

    u, f = iterate[0], source[0]
    kap_cols = jnp.pad(diffusivity.reshape(lanes, nx).T, ((depth, depth), (0, 0)))
    kap_cols = lax.dynamic_slice_in_dim(kap_cols, chip * own, own + 2 * depth, axis=0)
    edge = jnp.where(core == 0, u[nz - 1], u[0])
    swap = [(0, 1), (1, 0)]
    got = lax.ppermute(jnp.concatenate([edge, kap_cols], axis=0), "space", swap)
    got_edge, kap_other = got[:ny], got[ny:]
    zero = jnp.zeros_like(got_edge)
    before = jnp.where(core == 0, zero, got_edge)
    after = jnp.where(core == 0, got_edge, zero)
    padded = jnp.concatenate([before[None], u, after[None]], axis=0)
    s = f - diffusivity * (6.0 * u - neighbour_sum(padded))
    kap = jnp.where(
        core == 0,
        jnp.stack([kap_cols, kap_other], axis=1),
        jnp.stack([kap_other, kap_cols], axis=1),
    ).reshape(-1, lanes)
    lam = lax.dynamic_index_in_dim(
        jnp.asarray(lams), lax.axis_index(ROW), axis=0, keepdims=False
    )
    lam = jnp.broadcast_to(lam[:, :, None], (3, here, lanes))

    send = jnp.stack([u.reshape(lanes, nx).T, s.reshape(lanes, nx).T], axis=1)
    cells = lax.all_to_all(send, TM, split_axis=0, concat_axis=0, tiled=True)
    high = lax.Precision.HIGHEST
    first = jnp.dot(first_mat, cells.reshape(2 * total, lanes), precision=high)
    hist_u = first[:total]
    spec = first[total:].reshape(owners, 2 * here, lanes)
    residual = cells[:, 1] - hist_u

    spec = lax.all_to_all(spec, ROW, split_axis=0, concat_axis=0, tiled=True)
    spec = spec.reshape(own, cores, 2 * here, lanes)
    rest = depth - own

    def shifted(value, offset):
        pairs = [(i, i + offset) for i in range(chips) if 0 <= i + offset < chips]
        return lax.ppermute(value, CHIPS, pairs)

    left_near = shifted(spec, 1)
    right_near = shifted(spec, -1)
    left_far = shifted(spec[own - rest :], 2)
    right_far = shifted(spec[:rest], -2)
    back = make_sweeps(own, depth, here, lanes, ny)(
        left_far, left_near, spec, right_near, right_far, kap, lam
    )
    back = lax.all_to_all(back, ROW, split_axis=0, concat_axis=0, tiled=True)
    second = jnp.dot(second_mat, back.reshape(2 * total, lanes), precision=high)
    second = second.reshape(total, 2, lanes)
    image = second[:, 1]
    inner_ri = jnp.sum(residual * image)
    inner_ii = jnp.sum(image * image)
    lane = jnp.arange(lanes, dtype=jnp.int32)
    sums = jnp.where(lane == 0, inner_ri, jnp.where(lane == 1, inner_ii, 0.0))
    sums = jnp.broadcast_to(sums[None, None, :], (total, 1, lanes))
    send = jnp.concatenate([second, hist_u[:, None], sums], axis=1)
    times = lax.all_to_all(send, TM, split_axis=0, concat_axis=0, tiled=True)
    sums = jnp.sum(times[:, 3, :], axis=0, keepdims=True)
    sums = sums + lax.ppermute(sums, "space", swap)
    step = sums[0, 0] / sums[0, 1]

    def slab(index):
        return times[:, index].T.reshape(nz, ny, nx)

    new_iterate = u + step * slab(0)
    new_residual = s - slab(2) - step * slab(1)
    return (new_iterate[None], new_residual[None])


def solution(mesh):
    split = Mesh(
        mesh.devices.reshape(mesh.shape["groups"], 32, 4, mesh.shape["space"]),
        ("groups", "tm_0", "tm_1", "space"),
    )
    placed = (
        P(GROUPS_TM, "space", None, None),
        P(GROUPS_TM, "space", None, None),
        P(("groups", "space"), None, None),
    )
    return jax.shard_map(
        on_device,
        mesh=split,
        in_specs=placed,
        out_specs=(P(GROUPS_TM, "space", None, None), P(GROUPS_TM, "space", None, None)),
        check_vma=False,
    )
```

```python
import math

import jax
import jax.numpy as jnp
import numpy as np
from jax import lax
from jax.experimental import pallas as pl
from jax.experimental.pallas import tpu as pltpu
from jax.sharding import Mesh
from jax.sharding import PartitionSpec as P

SWEEPS = 6
TM = ("blocks", "pair", "tm_1")
ROW = ("pair", "tm_1", "space")
GROUPS_TM = ("groups", "blocks", "pair", "tm_1")
HIGH = lax.Precision.HIGHEST

frac_order = 0.3
step_length = 0.01
gamma_factor = 0.9086387328532904


def history_weights(count):
    k = np.arange(count + 1, dtype=np.float64) ** (1.0 - frac_order)
    b = k[1:] - k[:-1]
    d = np.concatenate([[1.0], b[1:] - b[:-1]])
    return d / (step_length**frac_order * gamma_factor)


def tables(total, owners):
    half = total // 2
    here = half // owners
    n = np.arange(total)
    d = history_weights(total)
    lag = n[:, None] - n[None, :]
    hist = np.where(lag >= 0, d[np.maximum(lag, 0)], 0.0)
    first = np.where(n < half, d, 0.0)
    angle = 2.0 * math.pi * ((n[:, None] * n[None, :]) % total) / total
    lam = (first[None, :] * np.exp(-1j * angle)).sum(1)
    fwd = np.zeros((owners, 2, here, total))
    inv = np.zeros((total, owners, 2, here))
    lams = np.zeros((owners, 2, 2, here))
    for q in range(owners):
        for j in range(here):
            k = q * here + j
            if k == 0:
                fwd[q, 0, j] = 1.0
                fwd[q, 1, j] = np.cos(angle[half])
                inv[:, q, 0, j] = 1.0 / total
                inv[:, q, 1, j] = np.cos(angle[half]) / total
                lams[q, 0, :, j] = lam[0].real, lam[half].real
            else:
                fwd[q, 0, j] = np.cos(angle[k])
                fwd[q, 1, j] = -np.sin(angle[k])
                inv[:, q, 0, j] = 2.0 * np.cos(angle[k]) / total
                inv[:, q, 1, j] = -2.0 * np.sin(angle[k]) / total
                lams[q, 0, :, j] = lam[k].real
                lams[q, 1, :, j] = lam[k].imag
    fwd = fwd.reshape(total, total)
    first_mat = np.zeros((2, total, total, 2))
    first_mat[0, :, :, 0] = hist
    first_mat[1, :, :, 0] = -fwd @ hist
    first_mat[1, :, :, 1] = fwd
    flat = inv.reshape(total, total)
    second_mat = np.zeros((2, total, owners, 2, 2 * here))
    second_mat[0, :, :, 0] = flat.reshape(total, owners, 2 * here)
    second_mat[1, :, :, 0] = (hist @ flat).reshape(total, owners, 2 * here)
    second_mat[1, :, :, 1] = flat.reshape(total, owners, 2 * here)
    f32 = np.float32
    return (
        first_mat.reshape(2 * total, 2 * total).astype(f32),
        second_mat.reshape(2 * total, 2 * total).astype(f32),
        lams.reshape(owners, 2, 2 * here).astype(f32),
    )


def local_call(kernel, name, outs, inputs, scratch=()):
    vmem = pl.BlockSpec(memory_space=pltpu.VMEM)
    return pl.pallas_call(
        kernel,
        out_shape=[jax.ShapeDtypeStruct(shape, jnp.float32) for shape in outs],
        in_specs=[vmem] * inputs,
        out_specs=[vmem] * len(outs),
        scratch_shapes=list(scratch),
        name=name,
    )


def iota(shape, dim):
    return lax.broadcasted_iota(jnp.int32, shape, dim)


def make_entry(nz, ny, nx):
    lanes = nz * ny

    def kernel(u, f, kappa, before, after, s, out):
        row, lane = iota((ny, nx), 0), iota((ny, nx), 1)
        for z in range(nz):
            v = u[z]
            near = (before[...] if z == 0 else u[z - 1]) + (after[...] if z == nz - 1 else u[z + 1])
            near = near + jnp.where(row == 0, 0.0, pltpu.roll(v, 1, 0))
            near = near + jnp.where(row == ny - 1, 0.0, pltpu.roll(v, ny - 1, 0))
            near = near + jnp.where(lane == 0, 0.0, pltpu.roll(v, 1, 1))
            near = near + jnp.where(lane == nx - 1, 0.0, pltpu.roll(v, nx - 1, 1))
            s[z] = f[z] - kappa[z] * (6.0 * v - near)
        out[pl.ds(0, nx, stride=2), :] = u[...].reshape(lanes, nx).T
        out[pl.ds(1, nx, stride=2), :] = s[...].reshape(lanes, nx).T

    return local_call(kernel, "entry", [(nz, ny, nx), (2 * nx, lanes)], 5)


def make_forward(total, lanes):
    def kernel(mat, cells, hist, spec):
        both = jnp.dot(mat[...], cells[...], precision=HIGH, preferred_element_type=jnp.float32)
        hist[...] = both[:total]
        spec[...] = both[total:]

    return local_call(kernel, "forward", [(total, lanes)] * 2, 2)


def make_backward(total, lanes):
    def kernel(mat, back, hist, cells, out):
        both = jnp.dot(mat[...], back[...], precision=HIGH, preferred_element_type=jnp.float32)
        image = both[total:]
        residual = cells[pl.ds(1, total, stride=2), :] - hist[...]
        ri = jnp.sum(residual * image, axis=0, keepdims=True)
        ii = jnp.sum(image * image, axis=0, keepdims=True)
        low = iota((1, lanes), 1) < lanes // 2
        sums = jnp.where(low, ri + pltpu.roll(ri, lanes // 2, 1), ii + pltpu.roll(ii, lanes // 2, 1))
        out[pl.ds(0, total, stride=4), :] = both[:total]
        out[pl.ds(1, total, stride=4), :] = image
        out[pl.ds(2, total, stride=4), :] = hist[...]
        out[pl.ds(3, total, stride=4), :] = jnp.broadcast_to(sums, (total, lanes))

    return local_call(kernel, "backward", [(4 * total, lanes)], 4)


def make_exit(nz, ny, nx):
    lanes = nz * ny

    def kernel(times, sums, u, s, new_u, new_r):
        low = iota((1, lanes), 1) < lanes // 2
        ri = jnp.sum(jnp.where(low, sums[...], 0.0), axis=1, keepdims=True)
        ii = jnp.sum(jnp.where(low, 0.0, sums[...]), axis=1, keepdims=True)
        step = (ri / ii).reshape(1, 1, 1)

        def slab(k):
            return times[pl.ds(k, nx, stride=4), :].T.reshape(nz, ny, nx)

        new_u[...] = u[...] + step * slab(0)
        new_r[...] = s[...] - slab(2) - step * slab(1)

    return local_call(kernel, "exit", [(nz, ny, nx)] * 2, 4)


def make_sweeps(own, depth, rows, lanes, ny):
    cols = own + 2 * depth
    shape = (rows, lanes)

    def kernel(left, mid, right, kap, lam, out, start, same, cross, ping, pong):
        flat = [(ref, c) for ref in (left, mid, right) for c in range(ref.shape[0])]
        lane = iota(shape, 1)
        y = lane % ny
        y_first, y_last = y == 0, y == ny - 1
        z_first, z_last = lane < ny, lane >= lanes - ny
        sign = jnp.where(iota(shape, 0) < rows // 2, -1.0, 1.0)
        lam_r, lam_i = lam[0], lam[1]
        lam_ii = lam_i * lam_i

        def swap(v):
            return pltpu.roll(v, rows // 2, 0)

        for c in range(cols):
            ref, at = flat[c]
            for h in range(2):
                k = jnp.broadcast_to(kap[2 * c + h : 2 * c + h + 1, :], shape)
                diag = lam_r + 6.0 * k
                over = 1.0 / (diag * diag + lam_ii)
                g = diag * over
                g_cross = sign * (-lam_i * over)
                spec = ref[at, h]
                first = g * spec + g_cross * swap(spec)
                start[c, h] = first
                ping[c, h] = first
                same[c, h] = g * k
                cross[c, h] = g_cross * k

        def around(buf, c):
            a, b = buf[c, 0], buf[c, 1]
            down_a, down_b = pltpu.roll(a, ny, 1), pltpu.roll(b, ny, 1)
            up_a, up_b = pltpu.roll(a, lanes - ny, 1), pltpu.roll(b, lanes - ny, 1)

            def along_y(v):
                return jnp.where(y_first, 0.0, pltpu.roll(v, 1, 1)) + jnp.where(
                    y_last, 0.0, pltpu.roll(v, lanes - 1, 1)
                )

            na = jnp.where(z_first, 0.0, down_a) + jnp.where(z_last, up_b, up_a) + along_y(a)
            nb = jnp.where(z_first, down_a, down_b) + jnp.where(z_last, 0.0, up_b) + along_y(b)
            return (
                na + buf[c - 1, 0] + buf[c + 1, 0],
                nb + buf[c - 1, 1] + buf[c + 1, 1],
            )

        now, then = ping, pong
        for sweep in range(1, SWEEPS):
            for c in range(sweep, cols - sweep):
                near = around(now, c)
                for h in range(2):
                    n = near[h]
                    then[c, h] = start[c, h] + (same[c, h] * n + cross[c, h] * swap(n))
            now, then = then, now
        for c in range(depth, depth + own):
            near = around(now, c)
            for h in range(2):
                sol = now[c, h]
                k = jnp.broadcast_to(kap[2 * c + h : 2 * c + h + 1, :], shape)
                row = 2 * (c - depth) + h
                out[row, 0] = sol
                out[row, 1] = k * (6.0 * sol - near[h])

    field = pltpu.VMEM((cols, 2, rows, lanes), jnp.float32)
    return local_call(kernel, "sweeps", [(2 * own, 2, rows, lanes)], 5, [field] * 5)


def on_device(iterate, source, diffusivity):
    _, nz, ny, nx = iterate.shape
    lanes = nz * ny
    blocks, pair = lax.axis_size("blocks"), lax.axis_size("pair")
    own = pair * lax.axis_size("tm_1")
    cores = lax.axis_size("space")
    total = blocks * own
    owners = own * cores
    rows = total // owners
    depth = SWEEPS
    first_mat, second_mat, lams = tables(total, owners)
    core = lax.axis_index("space")
    block = lax.axis_index("blocks")
    swap = [(0, 1), (1, 0)]

    u, f = iterate[0], source[0]
    got = lax.ppermute(jnp.where(core == 0, u[nz - 1], u[0]), "space", swap)
    before = jnp.where(core == 0, 0.0, got)
    after = jnp.where(core == 0, got, 0.0)
    s, send = make_entry(nz, ny, nx)(u, f, diffusivity, before, after)
    cells = lax.all_to_all(
        send.reshape(total, 2, lanes), TM, split_axis=0, concat_axis=0, tiled=True
    ).reshape(2 * total, lanes)

    kap = jnp.pad(diffusivity.reshape(lanes, nx).T, ((depth, depth), (0, 0)))
    kap = lax.dynamic_slice_in_dim(kap, block * own, own + 2 * depth, axis=0)
    kap_other = lax.ppermute(kap, "space", swap)
    kap = jnp.where(
        core == 0, jnp.stack([kap, kap_other], axis=1), jnp.stack([kap_other, kap], axis=1)
    ).reshape(-1, lanes)
    lam = lax.dynamic_index_in_dim(jnp.asarray(lams), lax.axis_index(ROW), axis=0, keepdims=False)
    lam = jnp.broadcast_to(lam[:, :, None], (2, rows, lanes))

    hist_u, spec = make_forward(total, lanes)(first_mat, cells)
    spec = lax.all_to_all(
        spec.reshape(owners, rows, lanes), ROW, split_axis=0, concat_axis=0, tiled=True
    ).reshape(own, cores, rows, lanes)

    def shifted(value, offset):
        pairs = [(i, i + offset) for i in range(blocks) if 0 <= i + offset < blocks]
        return lax.ppermute(value, "blocks", pairs)

    left = shifted(spec[own - depth :], 1)
    right = shifted(spec[:depth], -1)
    (back,) = make_sweeps(own, depth, rows, lanes, ny)(left, spec, right, kap, lam)
    back = lax.all_to_all(back, ROW, split_axis=0, concat_axis=0, tiled=True)
    (send,) = make_backward(total, lanes)(second_mat, back.reshape(2 * total, lanes), hist_u, cells)
    times = lax.all_to_all(
        send.reshape(total, 4, lanes), TM, split_axis=0, concat_axis=0, tiled=True
    )
    sums = jnp.sum(times[:, 3, :], axis=0, keepdims=True)
    sums = sums + lax.ppermute(sums, "space", swap)
    new_iterate, new_residual = make_exit(nz, ny, nx)(
        times.reshape(4 * total, lanes), sums, u, s
    )
    return (new_iterate[None], new_residual[None])


def solution(mesh):
    split = Mesh(
        mesh.devices.reshape(mesh.shape["groups"], 16, 2, 4, mesh.shape["space"]),
        ("groups", "blocks", "pair", "tm_1", "space"),
    )
    placed = (
        P(GROUPS_TM, "space", None, None),
        P(GROUPS_TM, "space", None, None),
        P(("groups", "space"), None, None),
    )
    return jax.shard_map(
        on_device,
        mesh=split,
        in_specs=placed,
        out_specs=(P(GROUPS_TM, "space", None, None), P(GROUPS_TM, "space", None, None)),
        check_vma=False,
    )
```

```python
import math

import jax
import jax.numpy as jnp
import numpy as np
from jax import lax
from jax.experimental import pallas as pl
from jax.experimental.pallas import tpu as pltpu
from jax.sharding import Mesh
from jax.sharding import PartitionSpec as P

SWEEPS = 6
TM = ("blocks", "pair", "tm_1")
ROW = ("pair", "tm_1", "space")
GROUPS_TM = ("groups", "blocks", "pair", "tm_1")
HIGH = lax.Precision.HIGHEST

frac_order = 0.3
step_length = 0.01
gamma_factor = 0.9086387328532904


def history_weights(count):
    k = np.arange(count + 1, dtype=np.float64) ** (1.0 - frac_order)
    b = k[1:] - k[:-1]
    d = np.concatenate([[1.0], b[1:] - b[:-1]])
    return d / (step_length**frac_order * gamma_factor)


def tables(total, owners):
    half = total // 2
    here = half // owners
    n = np.arange(total)
    d = history_weights(total)
    lag = n[:, None] - n[None, :]
    hist = np.where(lag >= 0, d[np.maximum(lag, 0)], 0.0)
    first = np.where(n < half, d, 0.0)
    angle = 2.0 * math.pi * ((n[:, None] * n[None, :]) % total) / total
    lam = (first[None, :] * np.exp(-1j * angle)).sum(1)
    fwd = np.zeros((owners, 2, here, total))
    inv = np.zeros((total, owners, 2, here))
    lams = np.zeros((owners, 2, 2, here))
    for q in range(owners):
        for j in range(here):
            k = q * here + j
            if k == 0:
                fwd[q, 0, j] = 1.0
                fwd[q, 1, j] = np.cos(angle[half])
                inv[:, q, 0, j] = 1.0 / total
                inv[:, q, 1, j] = np.cos(angle[half]) / total
                lams[q, 0, :, j] = lam[0].real, lam[half].real
            else:
                fwd[q, 0, j] = np.cos(angle[k])
                fwd[q, 1, j] = -np.sin(angle[k])
                inv[:, q, 0, j] = 2.0 * np.cos(angle[k]) / total
                inv[:, q, 1, j] = -2.0 * np.sin(angle[k]) / total
                lams[q, 0, :, j] = lam[k].real
                lams[q, 1, :, j] = lam[k].imag
    fwd = fwd.reshape(total, total)
    first_mat = np.zeros((2, total, total, 2))
    first_mat[0, :, :, 0] = hist
    first_mat[1, :, :, 0] = -fwd @ hist
    first_mat[1, :, :, 1] = fwd
    flat = inv.reshape(total, total)
    second_mat = np.zeros((2, total, owners, 2, 2 * here))
    second_mat[0, :, :, 0] = flat.reshape(total, owners, 2 * here)
    second_mat[1, :, :, 0] = (hist @ flat).reshape(total, owners, 2 * here)
    second_mat[1, :, :, 1] = flat.reshape(total, owners, 2 * here)
    f32 = np.float32
    return (
        first_mat.reshape(2 * total, 2 * total).astype(f32),
        second_mat.reshape(2 * total, 2 * total).astype(f32),
        lams.reshape(owners, 2, 2 * here).astype(f32),
    )


def local_call(kernel, name, outs, inputs, scratch=(), keep_out=True):
    vmem = pl.BlockSpec(memory_space=pltpu.VMEM)
    made = pltpu.VMEM if keep_out else jax.ShapeDtypeStruct
    call = pl.pallas_call(
        kernel,
        out_shape=[made(shape, jnp.float32) for shape in outs],
        in_specs=[vmem] * inputs,
        out_specs=[vmem] * len(outs),
        scratch_shapes=list(scratch),
        name=name,
    )

    def placed(*args):
        return call(*(pltpu.with_memory_space_constraint(a, pltpu.VMEM) for a in args))

    return placed


def iota(shape, dim):
    return lax.broadcasted_iota(jnp.int32, shape, dim)


def make_entry(nz, ny, nx):
    lanes = nz * ny

    def kernel(u, f, kappa, before, after, s, out):
        row, lane = iota((ny, nx), 0), iota((ny, nx), 1)
        for z in range(nz):
            v = u[z]
            near = (before[...] if z == 0 else u[z - 1]) + (after[...] if z == nz - 1 else u[z + 1])
            near = near + jnp.where(row == 0, 0.0, pltpu.roll(v, 1, 0))
            near = near + jnp.where(row == ny - 1, 0.0, pltpu.roll(v, ny - 1, 0))
            near = near + jnp.where(lane == 0, 0.0, pltpu.roll(v, 1, 1))
            near = near + jnp.where(lane == nx - 1, 0.0, pltpu.roll(v, nx - 1, 1))
            s[z] = f[z] - kappa[z] * (6.0 * v - near)
        out[pl.ds(0, nx, stride=2), :] = u[...].reshape(lanes, nx).T
        out[pl.ds(1, nx, stride=2), :] = s[...].reshape(lanes, nx).T

    return local_call(kernel, "entry", [(nz, ny, nx), (2 * nx, lanes)], 5)


def make_forward(total, lanes):
    def kernel(mat, cells, hist, spec):
        both = jnp.dot(mat[...], cells[...], precision=HIGH, preferred_element_type=jnp.float32)
        hist[...] = both[:total]
        spec[...] = both[total:]

    return local_call(kernel, "forward", [(total, lanes)] * 2, 2)


def make_backward(total, lanes):
    def kernel(mat, back, hist, cells, out):
        both = jnp.dot(mat[...], back[...], precision=HIGH, preferred_element_type=jnp.float32)
        image = both[total:]
        residual = cells[pl.ds(1, total, stride=2), :] - hist[...]
        ri = jnp.sum(residual * image, axis=0, keepdims=True)
        ii = jnp.sum(image * image, axis=0, keepdims=True)
        low = iota((1, lanes), 1) < lanes // 2
        sums = jnp.where(low, ri + pltpu.roll(ri, lanes // 2, 1), ii + pltpu.roll(ii, lanes // 2, 1))
        out[pl.ds(0, total, stride=4), :] = both[:total]
        out[pl.ds(1, total, stride=4), :] = image
        out[pl.ds(2, total, stride=4), :] = hist[...]
        out[pl.ds(3, total, stride=4), :] = jnp.broadcast_to(sums, (total, lanes))

    return local_call(kernel, "backward", [(4 * total, lanes)], 4)


def make_exit(nz, ny, nx):
    lanes = nz * ny

    def kernel(times, sums, u, s, new_u, new_r):
        low = iota((1, lanes), 1) < lanes // 2
        ri = jnp.sum(jnp.where(low, sums[...], 0.0), axis=1, keepdims=True)
        ii = jnp.sum(jnp.where(low, 0.0, sums[...]), axis=1, keepdims=True)
        step = (ri / ii).reshape(1, 1, 1)

        def slab(k):
            return times[pl.ds(k, nx, stride=4), :].T.reshape(nz, ny, nx)

        new_u[...] = u[...] + step * slab(0)
        new_r[...] = s[...] - slab(2) - step * slab(1)

    return local_call(kernel, "exit", [(nz, ny, nx)] * 2, 4, keep_out=False)


def make_sweeps(own, depth, rows, lanes, ny):
    cols = own + 2 * depth
    shape = (rows, lanes)

    def kernel(left, mid, right, kap, lam, out, start, same, cross, ping, pong):
        flat = [(ref, c) for ref in (left, mid, right) for c in range(ref.shape[0])]
        lane = iota(shape, 1)
        y = lane % ny
        y_first, y_last = y == 0, y == ny - 1
        z_first, z_last = lane < ny, lane >= lanes - ny
        sign = jnp.where(iota(shape, 0) < rows // 2, -1.0, 1.0)
        lam_r, lam_i = lam[0], lam[1]
        lam_ii = lam_i * lam_i

        def swap(v):
            return pltpu.roll(v, rows // 2, 0)

        for c in range(cols):
            ref, at = flat[c]
            for h in range(2):
                k = jnp.broadcast_to(kap[2 * c + h : 2 * c + h + 1, :], shape)
                diag = lam_r + 6.0 * k
                over = 1.0 / (diag * diag + lam_ii)
                g = diag * over
                g_cross = sign * (-lam_i * over)
                spec = ref[at, h]
                first = g * spec + g_cross * swap(spec)
                start[c, h] = first
                ping[c, h] = first
                same[c, h] = g * k
                cross[c, h] = g_cross * k

        def around(buf, c):
            a, b = buf[c, 0], buf[c, 1]
            down_a, down_b = pltpu.roll(a, ny, 1), pltpu.roll(b, ny, 1)
            up_a, up_b = pltpu.roll(a, lanes - ny, 1), pltpu.roll(b, lanes - ny, 1)

            def along_y(v):
                return jnp.where(y_first, 0.0, pltpu.roll(v, 1, 1)) + jnp.where(
                    y_last, 0.0, pltpu.roll(v, lanes - 1, 1)
                )

            na = jnp.where(z_first, 0.0, down_a) + jnp.where(z_last, up_b, up_a) + along_y(a)
            nb = jnp.where(z_first, down_a, down_b) + jnp.where(z_last, 0.0, up_b) + along_y(b)
            return (
                na + buf[c - 1, 0] + buf[c + 1, 0],
                nb + buf[c - 1, 1] + buf[c + 1, 1],
            )

        now, then = ping, pong
        for sweep in range(1, SWEEPS):
            for c in range(sweep, cols - sweep):
                near = around(now, c)
                for h in range(2):
                    n = near[h]
                    then[c, h] = start[c, h] + (same[c, h] * n + cross[c, h] * swap(n))
            now, then = then, now
        for c in range(depth, depth + own):
            near = around(now, c)
            for h in range(2):
                sol = now[c, h]
                k = jnp.broadcast_to(kap[2 * c + h : 2 * c + h + 1, :], shape)
                row = 2 * (c - depth) + h
                out[row, 0] = sol
                out[row, 1] = k * (6.0 * sol - near[h])

    field = pltpu.VMEM((cols, 2, rows, lanes), jnp.float32)
    return local_call(kernel, "sweeps", [(2 * own, 2, rows, lanes)], 5, [field] * 5)


def on_device(iterate, source, diffusivity):
    _, nz, ny, nx = iterate.shape
    lanes = nz * ny
    blocks, pair = lax.axis_size("blocks"), lax.axis_size("pair")
    own = pair * lax.axis_size("tm_1")
    cores = lax.axis_size("space")
    total = blocks * own
    owners = own * cores
    rows = total // owners
    depth = SWEEPS
    first_mat, second_mat, lams = tables(total, owners)
    core = lax.axis_index("space")
    block = lax.axis_index("blocks")
    swap = [(0, 1), (1, 0)]

    u, f = iterate[0], source[0]
    got = lax.ppermute(jnp.where(core == 0, u[nz - 1], u[0]), "space", swap)
    before = jnp.where(core == 0, 0.0, got)
    after = jnp.where(core == 0, got, 0.0)
    s, send = make_entry(nz, ny, nx)(u, f, diffusivity, before, after)
    cells = lax.all_to_all(
        send.reshape(total, 2, lanes), TM, split_axis=0, concat_axis=0, tiled=True
    ).reshape(2 * total, lanes)

    kap = jnp.pad(diffusivity.reshape(lanes, nx).T, ((depth, depth), (0, 0)))
    kap = lax.dynamic_slice_in_dim(kap, block * own, own + 2 * depth, axis=0)
    kap_other = lax.ppermute(kap, "space", swap)
    kap = jnp.where(
        core == 0, jnp.stack([kap, kap_other], axis=1), jnp.stack([kap_other, kap], axis=1)
    ).reshape(-1, lanes)
    lam = lax.dynamic_index_in_dim(jnp.asarray(lams), lax.axis_index(ROW), axis=0, keepdims=False)
    lam = jnp.broadcast_to(lam[:, :, None], (2, rows, lanes))
    cells, kap, lam = lax.optimization_barrier((cells, kap, lam))

    hist_u, spec = make_forward(total, lanes)(first_mat, cells)
    spec = lax.all_to_all(
        spec.reshape(owners, rows, lanes), ROW, split_axis=0, concat_axis=0, tiled=True
    ).reshape(own, cores, rows, lanes)

    def shifted(value, offset):
        pairs = [(i, i + offset) for i in range(blocks) if 0 <= i + offset < blocks]
        return lax.ppermute(value, "blocks", pairs)

    left = shifted(spec[own - depth :], 1)
    right = shifted(spec[:depth], -1)
    (back,) = make_sweeps(own, depth, rows, lanes, ny)(left, spec, right, kap, lam)
    back = lax.all_to_all(back, ROW, split_axis=0, concat_axis=0, tiled=True)
    (send,) = make_backward(total, lanes)(second_mat, back.reshape(2 * total, lanes), hist_u, cells)
    times = lax.all_to_all(
        send.reshape(total, 4, lanes), TM, split_axis=0, concat_axis=0, tiled=True
    )
    sums = jnp.sum(times[:, 3, :], axis=0, keepdims=True)
    sums = sums + lax.ppermute(sums, "space", swap)
    new_iterate, new_residual = make_exit(nz, ny, nx)(
        times.reshape(4 * total, lanes), sums, u, s
    )
    return (new_iterate[None], new_residual[None])


def solution(mesh):
    split = Mesh(
        mesh.devices.reshape(mesh.shape["groups"], 16, 2, 4, mesh.shape["space"]),
        ("groups", "blocks", "pair", "tm_1", "space"),
    )
    placed = (
        P(GROUPS_TM, "space", None, None),
        P(GROUPS_TM, "space", None, None),
        P(("groups", "space"), None, None),
    )
    return jax.shard_map(
        on_device,
        mesh=split,
        in_specs=placed,
        out_specs=(P(GROUPS_TM, "space", None, None), P(GROUPS_TM, "space", None, None)),
        check_vma=False,
    )
```

```python
import math

import jax
import jax.numpy as jnp
import numpy as np
from jax import lax
from jax.experimental import pallas as pl
from jax.experimental.pallas import tpu as pltpu
from jax.sharding import Mesh
from jax.sharding import PartitionSpec as P


SWEEPS = 6
TM = ("blocks", "pair", "tm_1")
ROW = ("pair", "tm_1", "space")
GROUPS_TM = ("groups", "blocks", "pair", "tm_1")
HIGH = lax.Precision.HIGHEST

frac_order = 0.3
step_length = 0.01
gamma_factor = 0.9086387328532904


def history_weights(count):
    k = np.arange(count + 1, dtype=np.float64) ** (1.0 - frac_order)
    b = k[1:] - k[:-1]
    d = np.concatenate([[1.0], b[1:] - b[:-1]])
    return d / (step_length**frac_order * gamma_factor)


def tables(total, owners):
    half = total // 2
    here = half // owners
    n = np.arange(total)
    d = history_weights(total)
    lag = n[:, None] - n[None, :]
    hist = np.where(lag >= 0, d[np.maximum(lag, 0)], 0.0)
    first = np.where(n < half, d, 0.0)
    angle = 2.0 * math.pi * ((n[:, None] * n[None, :]) % total) / total
    lam = (first[None, :] * np.exp(-1j * angle)).sum(1)
    fwd = np.zeros((owners, 2, here, total))
    inv = np.zeros((total, owners, 2, here))
    lams = np.zeros((owners, 2, 2, here))
    for q in range(owners):
        for j in range(here):
            k = q * here + j
            if k == 0:
                fwd[q, 0, j] = 1.0
                fwd[q, 1, j] = np.cos(angle[half])
                inv[:, q, 0, j] = 1.0 / total
                inv[:, q, 1, j] = np.cos(angle[half]) / total
                lams[q, 0, :, j] = lam[0].real, lam[half].real
            else:
                fwd[q, 0, j] = np.cos(angle[k])
                fwd[q, 1, j] = -np.sin(angle[k])
                inv[:, q, 0, j] = 2.0 * np.cos(angle[k]) / total
                inv[:, q, 1, j] = -2.0 * np.sin(angle[k]) / total
                lams[q, 0, :, j] = lam[k].real
                lams[q, 1, :, j] = lam[k].imag
    fwd = fwd.reshape(total, total)
    first_mat = np.zeros((3 * total, total, 2))
    first_mat[:total, :, 0] = hist
    spectra = first_mat[total:].reshape(owners, 2, 2 * here, total, 2)
    spectra[:, 0, :, :, 0] = (-fwd @ hist).reshape(owners, 2 * here, total)
    spectra[:, 0, :, :, 1] = fwd.reshape(owners, 2 * here, total)
    spectra[:, 1, :, :, 0] = fwd.reshape(owners, 2 * here, total)
    flat = inv.reshape(total, total)
    second_mat = np.zeros((2, total, owners, 2, 2 * here))
    second_mat[0, :, :, 0] = flat.reshape(total, owners, 2 * here)
    second_mat[1, :, :, 0] = (hist @ flat).reshape(total, owners, 2 * here)
    second_mat[1, :, :, 1] = flat.reshape(total, owners, 2 * here)
    f32 = np.float32
    return (
        first_mat.reshape(3 * total, 2 * total).astype(f32),
        second_mat.reshape(2 * total, 2 * total).astype(f32),
        lams.reshape(owners, 2, 2 * here).astype(f32),
    )


def local_call(kernel, outs, inputs, scratch=(), keep_in=True, keep_out=True):
    vmem = pl.BlockSpec(memory_space=pltpu.VMEM)
    made = pltpu.VMEM if keep_out else jax.ShapeDtypeStruct
    call = pl.pallas_call(
        kernel,
        out_shape=[made(shape, jnp.float32) for shape in outs],
        in_specs=[vmem] * inputs,
        out_specs=[vmem] * len(outs),
        scratch_shapes=list(scratch),
    )

    def placed(*args):
        if keep_in:
            args = [pltpu.with_memory_space_constraint(a, pltpu.VMEM) for a in args]
        return call(*args)

    return placed


def iota(shape, dim):
    return lax.broadcasted_iota(jnp.int32, shape, dim)


def make_entry(nz, ny, nx):
    lanes = nz * ny

    def kernel(u, f, kappa, s, out):
        row, lane = iota((ny, nx), 0), iota((ny, nx), 1)
        for z in range(nz):
            v = u[z]
            near = jnp.where(row == 0, 0.0, pltpu.roll(v, 1, 0))
            near = near + jnp.where(row == ny - 1, 0.0, pltpu.roll(v, ny - 1, 0))
            near = near + jnp.where(lane == 0, 0.0, pltpu.roll(v, 1, 1))
            near = near + jnp.where(lane == nx - 1, 0.0, pltpu.roll(v, nx - 1, 1))
            if z > 0:
                near = near + u[z - 1]
            if z < nz - 1:
                near = near + u[z + 1]
            s[z] = f[z] - kappa[z] * (6.0 * v - near)
        out[pl.ds(0, nx, stride=2), :] = u[...].reshape(lanes, nx).T
        out[pl.ds(1, nx, stride=2), :] = s[...].reshape(lanes, nx).T

    return local_call(kernel, [(nz, ny, nx), (2 * nx, lanes)], 3, keep_in=False)


def make_forward(total, lanes, ny):
    def kernel(mat, cells, masks, hist, spec, edge):
        out = jnp.dot(mat[...], cells[...], precision=HIGH, preferred_element_type=jnp.float32)
        hist[...] = out[:total]
        spec[...] = out[total:]
        u = cells[pl.ds(0, total, stride=2), :]
        edge[...] = masks[0:1, :] * pltpu.roll(u, ny, 1) + masks[1:2, :] * pltpu.roll(
            u, lanes - ny, 1
        )

    return local_call(kernel, [(total, lanes), (2 * total, lanes), (total, lanes)], 3)


def make_border(own, depth, rows, lanes, ny):
    def kernel(spec, kap, out, to_right, to_left):
        lane = iota((rows, lanes), 1)
        first, last = lane < ny, lane >= lanes - ny
        for c in range(own):
            for h in range(2):
                at = 2 * (depth + c) + h
                k = jnp.broadcast_to(kap[at : at + 1, :], (rows, lanes))
                other = pltpu.roll(spec[c, 1 - h, rows:, :], ny if h else lanes - ny, 1)
                value = spec[c, h, :rows, :] + jnp.where(first if h else last, k * other, 0.0)
                out[c, h] = value
                if c >= own - depth:
                    to_right[c - (own - depth), h] = value
                if c < depth:
                    to_left[c, h] = value

    shapes = [(count, 2, rows, lanes) for count in (own, depth, depth)]
    return local_call(kernel, shapes, 2)


def make_backward(total, lanes):
    def kernel(mat, back, hist, cells, edge, kap, out):
        both = jnp.dot(mat[...], back[...], precision=HIGH, preferred_element_type=jnp.float32)
        image = both[total:]
        residual = cells[pl.ds(1, total, stride=2), :] - hist[...] + kap[...] * edge[...]
        ri = jnp.sum(residual * image, axis=0, keepdims=True)
        ii = jnp.sum(image * image, axis=0, keepdims=True)
        low = iota((1, lanes), 1) < lanes // 2
        sums = jnp.where(low, ri + pltpu.roll(ri, lanes // 2, 1), ii + pltpu.roll(ii, lanes // 2, 1))
        out[pl.ds(0, total, stride=4), :] = both[:total]
        out[pl.ds(1, total, stride=4), :] = image
        out[pl.ds(2, total, stride=4), :] = hist[...]
        out[pl.ds(3, total, stride=4), :] = jnp.broadcast_to(sums, (total, lanes))

    return local_call(kernel, [(4 * total, lanes)], 6)


def make_exit(nz, ny, nx):
    lanes = nz * ny

    def kernel(times, sums, u, s, low_plane, high_plane, new_u, new_r):
        low = iota((1, lanes), 1) < lanes // 2
        ri = jnp.sum(jnp.where(low, sums[...], 0.0), axis=1, keepdims=True)
        ii = jnp.sum(jnp.where(low, 0.0, sums[...]), axis=1, keepdims=True)
        step = (ri / ii).reshape(1, 1, 1)

        def slab(k):
            return times[pl.ds(k, nx, stride=4), :].T.reshape(nz, ny, nx)

        new_u[...] = u[...] + step * slab(0)
        plane = s[...] - slab(2) - step * slab(1)
        new_r[...] = plane
        new_r[0] = plane[0] + low_plane[...]
        new_r[nz - 1] = plane[nz - 1] + high_plane[...]

    return local_call(kernel, [(nz, ny, nx)] * 2, 6, keep_out=False)


def make_sweeps(own, depth, rows, lanes, ny):
    cols = own + 2 * depth
    shape = (rows, lanes)

    def kernel(left, mid, right, kap, lam, out, start, same, cross, ping, pong):
        flat = [(ref, c) for ref in (left, mid, right) for c in range(ref.shape[0])]
        lane = iota(shape, 1)
        y = lane % ny
        y_first, y_last = y == 0, y == ny - 1
        z_first, z_last = lane < ny, lane >= lanes - ny
        sign = jnp.where(iota(shape, 0) < rows // 2, -1.0, 1.0)
        lam_r, lam_i = lam[0], lam[1]
        lam_ii = lam_i * lam_i

        def swap(v):
            return pltpu.roll(v, rows // 2, 0)

        for c in range(cols):
            ref, at = flat[c]
            for h in range(2):
                k = jnp.broadcast_to(kap[2 * c + h : 2 * c + h + 1, :], shape)
                diag = lam_r + 6.0 * k
                over = 1.0 / (diag * diag + lam_ii)
                g = diag * over
                g_cross = sign * (-lam_i * over)
                spec = ref[at, h]
                first = g * spec + g_cross * swap(spec)
                start[c, h] = first
                ping[c, h] = first
                same[c, h] = g * k
                cross[c, h] = g_cross * k

        def around(buf, c):
            a, b = buf[c, 0], buf[c, 1]
            down_a, down_b = pltpu.roll(a, ny, 1), pltpu.roll(b, ny, 1)
            up_a, up_b = pltpu.roll(a, lanes - ny, 1), pltpu.roll(b, lanes - ny, 1)

            def along_y(v):
                return jnp.where(y_first, 0.0, pltpu.roll(v, 1, 1)) + jnp.where(
                    y_last, 0.0, pltpu.roll(v, lanes - 1, 1)
                )

            na = jnp.where(z_first, 0.0, down_a) + jnp.where(z_last, up_b, up_a) + along_y(a)
            nb = jnp.where(z_first, down_a, down_b) + jnp.where(z_last, 0.0, up_b) + along_y(b)
            return (
                na + buf[c - 1, 0] + buf[c + 1, 0],
                nb + buf[c - 1, 1] + buf[c + 1, 1],
            )

        now, then = ping, pong
        for sweep in range(1, SWEEPS):
            for c in range(sweep, cols - sweep):
                near = around(now, c)
                for h in range(2):
                    n = near[h]
                    then[c, h] = start[c, h] + (same[c, h] * n + cross[c, h] * swap(n))
            now, then = then, now
        for c in range(depth, depth + own):
            near = around(now, c)
            for h in range(2):
                sol = now[c, h]
                k = jnp.broadcast_to(kap[2 * c + h : 2 * c + h + 1, :], shape)
                row = 2 * (c - depth) + h
                out[row, 0] = sol
                out[row, 1] = k * (6.0 * sol - near[h])

    field = pltpu.VMEM((cols, 2, rows, lanes), jnp.float32)
    return local_call(kernel, [(2 * own, 2, rows, lanes)], 5, [field] * 5)


def on_device(iterate, source, diffusivity):
    _, nz, ny, nx = iterate.shape
    lanes = nz * ny
    blocks, pair = lax.axis_size("blocks"), lax.axis_size("pair")
    own = pair * lax.axis_size("tm_1")
    cores = lax.axis_size("space")
    total = blocks * own
    owners = own * cores
    rows = total // owners
    depth = SWEEPS
    first_mat, second_mat, lams = tables(total, owners)
    core = lax.axis_index("space")
    block = lax.axis_index("blocks")
    swap = [(0, 1), (1, 0)]

    u, f = iterate[0], source[0]
    s, send = make_entry(nz, ny, nx)(u, f, diffusivity)
    send, u, diffusivity = lax.optimization_barrier((send, u, diffusivity))
    cells = lax.all_to_all(
        send.reshape(total, 2, lanes), TM, split_axis=0, concat_axis=0, tiled=True
    ).reshape(2 * total, lanes)

    kap = jnp.pad(diffusivity.reshape(lanes, nx).T, ((depth, depth), (0, 0)))
    kap = lax.dynamic_slice_in_dim(kap, block * own, own + 2 * depth, axis=0)
    my_kap = lax.dynamic_slice_in_dim(kap, depth + lax.axis_index(TM[1:]), 1, axis=0)
    edge = jnp.where(core == 0, u[nz - 1], u[0])
    got = lax.ppermute(jnp.concatenate([edge, kap], axis=0), "space", swap)
    got_edge, kap_other = got[:ny], got[ny:]
    kap = jnp.where(
        core == 0, jnp.stack([kap, kap_other], axis=1), jnp.stack([kap_other, kap], axis=1)
    ).reshape(-1, lanes)
    low_plane = jnp.where(core == 0, 0.0, diffusivity[0] * got_edge)
    high_plane = jnp.where(core == 0, diffusivity[nz - 1] * got_edge, 0.0)
    lane = jnp.arange(lanes, dtype=jnp.int32)
    masks = jnp.where(
        core == 0,
        jnp.stack([lane < ny, lane < 0]),
        jnp.stack([lane < 0, lane >= lanes - ny]),
    ).astype(jnp.float32)
    lam = lax.dynamic_index_in_dim(jnp.asarray(lams), lax.axis_index(ROW), axis=0, keepdims=False)
    lam = jnp.broadcast_to(lam[:, :, None], (2, rows, lanes))
    cells, kap, my_kap, low_plane, high_plane, masks, lam = lax.optimization_barrier(
        (cells, kap, my_kap, low_plane, high_plane, masks, lam)
    )

    hist_u, spec, edge_u = make_forward(total, lanes, ny)(first_mat, cells, masks)
    spec = lax.all_to_all(
        spec.reshape(owners, 2 * rows, lanes), ROW, split_axis=0, concat_axis=0, tiled=True
    )
    spec, to_right, to_left = make_border(own, depth, rows, lanes, ny)(
        spec.reshape(own, cores, 2 * rows, lanes), kap
    )

    to_right, to_left, edge_u = lax.optimization_barrier((to_right, to_left, edge_u))

    def shifted(value, offset):
        pairs = [(i, i + offset) for i in range(blocks) if 0 <= i + offset < blocks]
        return lax.ppermute(value, "blocks", pairs)

    left = shifted(to_right, 1)
    right = shifted(to_left, -1)
    edge_u = lax.ppermute(edge_u, "space", swap)
    left, right, edge_u = lax.optimization_barrier((left, right, edge_u))
    (back,) = make_sweeps(own, depth, rows, lanes, ny)(left, spec, right, kap, lam)
    back = lax.all_to_all(back, ROW, split_axis=0, concat_axis=0, tiled=True)
    (send,) = make_backward(total, lanes)(
        second_mat, back.reshape(2 * total, lanes), hist_u, cells, edge_u, my_kap
    )
    times = lax.all_to_all(
        send.reshape(total, 4, lanes), TM, split_axis=0, concat_axis=0, tiled=True
    )
    sums = jnp.sum(times[:, 3, :], axis=0, keepdims=True)
    sums = sums + lax.ppermute(sums, "space", swap)
    new_iterate, new_residual = make_exit(nz, ny, nx)(
        times.reshape(4 * total, lanes), sums, u, s, low_plane, high_plane
    )
    return (new_iterate[None], new_residual[None])


def solution(mesh):
    split = Mesh(
        mesh.devices.reshape(mesh.shape["groups"], 16, 2, 4, mesh.shape["space"]),
        ("groups", "blocks", "pair", "tm_1", "space"),
    )
    placed = (
        P(GROUPS_TM, "space", None, None),
        P(GROUPS_TM, "space", None, None),
        P(("groups", "space"), None, None),
    )
    return jax.shard_map(
        on_device,
        mesh=split,
        in_specs=placed,
        out_specs=(P(GROUPS_TM, "space", None, None), P(GROUPS_TM, "space", None, None)),
        check_vma=False,
    )
```

```python
import math

import jax
import jax.numpy as jnp
import numpy as np
from jax import lax
from jax.experimental import pallas as pl
from jax.experimental.pallas import tpu as pltpu
from jax.sharding import Mesh
from jax.sharding import PartitionSpec as P


SWEEPS = 6
TM = ("blocks", "pair", "tm_1")
ROW = ("pair", "tm_1", "space")
GROUPS_TM = ("groups", "blocks", "pair", "tm_1")
HIGH = lax.Precision.HIGHEST

frac_order = 0.3
step_length = 0.01
gamma_factor = 0.9086387328532904


def history_weights(count):
    k = np.arange(count + 1, dtype=np.float64) ** (1.0 - frac_order)
    b = k[1:] - k[:-1]
    d = np.concatenate([[1.0], b[1:] - b[:-1]])
    return d / (step_length**frac_order * gamma_factor)


def tables(total, owners):
    half = total // 2
    here = half // owners
    n = np.arange(total)
    d = history_weights(total)
    lag = n[:, None] - n[None, :]
    hist = np.where(lag >= 0, d[np.maximum(lag, 0)], 0.0)
    first = np.where(n < half, d, 0.0)
    angle = 2.0 * math.pi * ((n[:, None] * n[None, :]) % total) / total
    lam = (first[None, :] * np.exp(-1j * angle)).sum(1)
    fwd = np.zeros((owners, 2, here, total))
    inv = np.zeros((total, owners, 2, here))
    lams = np.zeros((owners, 2, 2, here))
    for q in range(owners):
        for j in range(here):
            k = q * here + j
            if k == 0:
                fwd[q, 0, j] = 1.0
                fwd[q, 1, j] = np.cos(angle[half])
                inv[:, q, 0, j] = 1.0 / total
                inv[:, q, 1, j] = np.cos(angle[half]) / total
                lams[q, 0, :, j] = lam[0].real, lam[half].real
            else:
                fwd[q, 0, j] = np.cos(angle[k])
                fwd[q, 1, j] = -np.sin(angle[k])
                inv[:, q, 0, j] = 2.0 * np.cos(angle[k]) / total
                inv[:, q, 1, j] = -2.0 * np.sin(angle[k]) / total
                lams[q, 0, :, j] = lam[k].real
                lams[q, 1, :, j] = lam[k].imag
    fwd = fwd.reshape(total, total)
    first_mat = np.zeros((2 * total, total, 2))
    spectra = first_mat.reshape(owners, 2, 2 * here, total, 2)
    spectra[:, 0, :, :, 0] = (-fwd @ hist).reshape(owners, 2 * here, total)
    spectra[:, 0, :, :, 1] = fwd.reshape(owners, 2 * here, total)
    spectra[:, 1, :, :, 0] = fwd.reshape(owners, 2 * here, total)
    flat = inv.reshape(total, owners, 2 * here)
    second_mat = np.zeros((3, total, owners, 3, 2 * here))
    second_mat[0, :, :, 0] = flat
    second_mat[1, :, :, 0] = (hist @ inv.reshape(total, total)).reshape(flat.shape)
    second_mat[1, :, :, 1] = flat
    second_mat[2, :, :, 2] = flat
    f32 = np.float32
    return (
        first_mat.reshape(2 * total, 2 * total).astype(f32),
        second_mat.reshape(3 * total, 3 * total).astype(f32),
        lams.reshape(owners, 2, 2 * here).astype(f32),
    )


def local_call(kernel, outs, inputs, scratch=(), keep_in=True, keep_out=True):
    vmem = pl.BlockSpec(memory_space=pltpu.VMEM)
    made = pltpu.VMEM if keep_out else jax.ShapeDtypeStruct
    call = pl.pallas_call(
        kernel,
        out_shape=[made(shape, jnp.float32) for shape in outs],
        in_specs=[vmem] * inputs,
        out_specs=[vmem] * len(outs),
        scratch_shapes=list(scratch),
    )

    def placed(*args):
        if keep_in:
            args = [pltpu.with_memory_space_constraint(a, pltpu.VMEM) for a in args]
        return call(*args)

    return placed


def iota(shape, dim):
    return lax.broadcasted_iota(jnp.int32, shape, dim)


def make_entry(nz, ny, nx):
    lanes = nz * ny

    def kernel(u, f, kappa, out, s):
        row, lane = iota((ny, nx), 0), iota((ny, nx), 1)
        for z in range(nz):
            v = u[z]
            near = jnp.where(row == 0, 0.0, pltpu.roll(v, 1, 0))
            near = near + jnp.where(row == ny - 1, 0.0, pltpu.roll(v, ny - 1, 0))
            near = near + jnp.where(lane == 0, 0.0, pltpu.roll(v, 1, 1))
            near = near + jnp.where(lane == nx - 1, 0.0, pltpu.roll(v, nx - 1, 1))
            if z > 0:
                near = near + u[z - 1]
            if z < nz - 1:
                near = near + u[z + 1]
            s[z] = f[z] - kappa[z] * (6.0 * v - near)
        out[pl.ds(0, nx, stride=2), :] = u[...].reshape(lanes, nx).T
        out[pl.ds(1, nx, stride=2), :] = s[...].reshape(lanes, nx).T

    scratch = [pltpu.VMEM((nz, ny, nx), jnp.float32)]
    return local_call(kernel, [(2 * nx, lanes)], 3, scratch, keep_in=False)


def make_forward(total, lanes):
    def kernel(mat, cells, spec):
        spec[...] = jnp.dot(
            mat[...], cells[...], precision=HIGH, preferred_element_type=jnp.float32
        )

    return local_call(kernel, [(2 * total, lanes)], 2)


def make_border(own, depth, rows, lanes, ny):
    def kernel(spec, kap, out, to_right, to_left):
        lane = iota((rows, lanes), 1)
        first, last = lane < ny, lane >= lanes - ny
        for c in range(own):
            for h in range(2):
                at = 2 * (depth + c) + h
                k = jnp.broadcast_to(kap[at : at + 1, :], (rows, lanes))
                other = pltpu.roll(spec[c, 1 - h, rows:, :], ny if h else lanes - ny, 1)
                value = spec[c, h, :rows, :] + jnp.where(first if h else last, k * other, 0.0)
                out[c, h] = value
                if c >= own - depth:
                    to_right[c - (own - depth), h] = value
                if c < depth:
                    to_left[c, h] = value

    shapes = [(count, 2, rows, lanes) for count in (own, depth, depth)]
    return local_call(kernel, shapes, 2)


def make_backward(total, lanes):
    def kernel(mat, back, out):
        fields = jnp.concatenate(
            [back[:, 3 * h : 3 * h + 3].reshape(3 * total, lanes) for h in range(2)], axis=1
        )
        every = jnp.dot(mat[...], fields, precision=HIGH, preferred_element_type=jnp.float32)
        image = every[total : 2 * total]
        ri = jnp.sum(every[2 * total :] * image, axis=0, keepdims=True)
        ii = jnp.sum(image * image, axis=0, keepdims=True)
        ri = ri[:, :lanes] + ri[:, lanes:]
        ii = ii[:, :lanes] + ii[:, lanes:]
        low = iota((1, lanes), 1) < lanes // 2
        sums = jnp.where(low, ri + pltpu.roll(ri, lanes // 2, 1), ii + pltpu.roll(ii, lanes // 2, 1))
        for k in range(3):
            out[pl.ds(k, total, stride=4), :] = every[k * total : (k + 1) * total, :lanes]
        out[pl.ds(3, total, stride=4), :] = jnp.broadcast_to(sums, (total, lanes))

    return local_call(kernel, [(4 * total, lanes)], 2)


def make_exit(nz, ny, nx):
    lanes = nz * ny

    def kernel(times, u, new_u, new_r):
        low = iota((1, lanes), 1) < lanes // 2
        row = jnp.sum(times[pl.ds(3, nx, stride=4), :], axis=0, keepdims=True)
        ri = jnp.sum(jnp.where(low, row, 0.0), axis=1, keepdims=True)
        ii = jnp.sum(jnp.where(low, 0.0, row), axis=1, keepdims=True)
        step = (ri / ii).reshape(1, 1, 1)

        def slab(k):
            return times[pl.ds(k, nx, stride=4), :].T.reshape(nz, ny, nx)

        new_u[...] = u[...] + step * slab(0)
        new_r[...] = slab(2) - step * slab(1)

    return local_call(kernel, [(nz, ny, nx)] * 2, 2, keep_out=False)


def make_sweeps(own, depth, rows, lanes, ny):
    cols = own + 2 * depth
    shape = (rows, lanes)

    def kernel(left, mid, right, kap, lam, out, start, same, cross, ping, pong):
        flat = [(ref, c) for ref in (left, mid, right) for c in range(ref.shape[0])]
        lane = iota(shape, 1)
        y = lane % ny
        y_first, y_last = y == 0, y == ny - 1
        z_first, z_last = lane < ny, lane >= lanes - ny
        sign = jnp.where(iota(shape, 0) < rows // 2, -1.0, 1.0)
        lam_r, lam_i = lam[0], lam[1]
        lam_ii = lam_i * lam_i

        def swap(v):
            return pltpu.roll(v, rows // 2, 0)

        for c in range(cols):
            ref, at = flat[c]
            for h in range(2):
                k = jnp.broadcast_to(kap[2 * c + h : 2 * c + h + 1, :], shape)
                diag = lam_r + 6.0 * k
                over = 1.0 / (diag * diag + lam_ii)
                g = diag * over
                g_cross = sign * (-lam_i * over)
                spec = ref[at, h]
                first = g * spec + g_cross * swap(spec)
                start[c, h] = first
                ping[c, h] = first
                same[c, h] = g * k
                cross[c, h] = g_cross * k

        def around(buf, c):
            a, b = buf[c, 0], buf[c, 1]
            down_a, down_b = pltpu.roll(a, ny, 1), pltpu.roll(b, ny, 1)
            up_a, up_b = pltpu.roll(a, lanes - ny, 1), pltpu.roll(b, lanes - ny, 1)

            def along_y(v):
                return jnp.where(y_first, 0.0, pltpu.roll(v, 1, 1)) + jnp.where(
                    y_last, 0.0, pltpu.roll(v, lanes - 1, 1)
                )

            na = jnp.where(z_first, 0.0, down_a) + jnp.where(z_last, up_b, up_a) + along_y(a)
            nb = jnp.where(z_first, down_a, down_b) + jnp.where(z_last, 0.0, up_b) + along_y(b)
            return (
                na + buf[c - 1, 0] + buf[c + 1, 0],
                nb + buf[c - 1, 1] + buf[c + 1, 1],
            )

        now, then = ping, pong
        for sweep in range(1, SWEEPS):
            for c in range(sweep, cols - sweep):
                near = around(now, c)
                for h in range(2):
                    n = near[h]
                    then[c, h] = start[c, h] + (same[c, h] * n + cross[c, h] * swap(n))
            now, then = then, now
        for c in range(depth, depth + own):
            near = around(now, c)
            for h in range(2):
                sol = now[c, h]
                k = jnp.broadcast_to(kap[2 * c + h : 2 * c + h + 1, :], shape)
                stiff = k * (6.0 * sol - near[h])
                for core in range(2):
                    row, at = 2 * (c - depth) + core, 0 if core == h else 3
                    out[row, at] = sol
                    out[row, at + 1] = stiff
                    out[row, at + 2] = mid[c - depth, h]

    field = pltpu.VMEM((cols, 2, rows, lanes), jnp.float32)
    return local_call(kernel, [(2 * own, 6, rows, lanes)], 5, [field] * 5)


def on_device(iterate, source, diffusivity):
    _, nz, ny, nx = iterate.shape
    lanes = nz * ny
    blocks, pair = lax.axis_size("blocks"), lax.axis_size("pair")
    own = pair * lax.axis_size("tm_1")
    cores = lax.axis_size("space")
    total = blocks * own
    owners = own * cores
    rows = total // owners
    depth = SWEEPS
    first_mat, second_mat, lams = tables(total, owners)
    core = lax.axis_index("space")
    block = lax.axis_index("blocks")
    swap = [(0, 1), (1, 0)]

    u, f = iterate[0], source[0]
    (send,) = make_entry(nz, ny, nx)(u, f, diffusivity)
    send, diffusivity = lax.optimization_barrier((send, diffusivity))
    cells = lax.all_to_all(
        send.reshape(total, 2, lanes), TM, split_axis=0, concat_axis=0, tiled=True
    ).reshape(2 * total, lanes)

    kap = jnp.pad(diffusivity.reshape(lanes, nx).T, ((depth, depth), (0, 0)))
    kap = lax.dynamic_slice_in_dim(kap, block * own, own + 2 * depth, axis=0)
    kap_other = lax.ppermute(kap, "space", swap)
    kap = jnp.where(
        core == 0, jnp.stack([kap, kap_other], axis=1), jnp.stack([kap_other, kap], axis=1)
    ).reshape(-1, lanes)
    lam = lax.dynamic_index_in_dim(jnp.asarray(lams), lax.axis_index(ROW), axis=0, keepdims=False)
    lam = jnp.broadcast_to(lam[:, :, None], (2, rows, lanes))
    cells, kap, lam = lax.optimization_barrier((cells, kap, lam))

    (spec,) = make_forward(total, lanes)(first_mat, cells)
    spec = lax.all_to_all(
        spec.reshape(owners, 2 * rows, lanes), ROW, split_axis=0, concat_axis=0, tiled=True
    )
    spec, to_right, to_left = make_border(own, depth, rows, lanes, ny)(
        spec.reshape(own, cores, 2 * rows, lanes), kap
    )

    def shifted(value, offset):
        pairs = [(i, i + offset) for i in range(blocks) if 0 <= i + offset < blocks]
        return lax.ppermute(value, "blocks", pairs)

    left = shifted(to_right, 1)
    right = shifted(to_left, -1)
    (back,) = make_sweeps(own, depth, rows, lanes, ny)(left, spec, right, kap, lam)
    back = lax.all_to_all(back, ROW, split_axis=0, concat_axis=0, tiled=True)
    (send,) = make_backward(total, lanes)(second_mat, back)
    times = lax.all_to_all(
        send.reshape(total, 4, lanes), TM, split_axis=0, concat_axis=0, tiled=True
    )
    new_iterate, new_residual = make_exit(nz, ny, nx)(times.reshape(4 * total, lanes), u)
    return (new_iterate[None], new_residual[None])


def solution(mesh):
    split = Mesh(
        mesh.devices.reshape(mesh.shape["groups"], 16, 2, 4, mesh.shape["space"]),
        ("groups", "blocks", "pair", "tm_1", "space"),
    )
    placed = (
        P(GROUPS_TM, "space", None, None),
        P(GROUPS_TM, "space", None, None),
        P(("groups", "space"), None, None),
    )
    return jax.shard_map(
        on_device,
        mesh=split,
        in_specs=placed,
        out_specs=(P(GROUPS_TM, "space", None, None), P(GROUPS_TM, "space", None, None)),
        check_vma=False,
    )
```

```python
import math

import jax
import jax.numpy as jnp
import numpy as np
from jax import lax
from jax.experimental import pallas as pl
from jax.experimental.pallas import tpu as pltpu
from jax.sharding import Mesh
from jax.sharding import PartitionSpec as P


SWEEPS = 6
TM = ("blocks", "pair", "tm_1")
ROW = ("pair", "tm_1", "space")
GROUPS_TM = ("groups", "blocks", "pair", "tm_1")
HIGH = lax.Precision.HIGHEST

frac_order = 0.3
step_length = 0.01
gamma_factor = 0.9086387328532904


def history_weights(count):
    k = np.arange(count + 1, dtype=np.float64) ** (1.0 - frac_order)
    b = k[1:] - k[:-1]
    d = np.concatenate([[1.0], b[1:] - b[:-1]])
    return d / (step_length**frac_order * gamma_factor)


def tables(total, owners, own):
    half = total // 2
    here = half // owners
    n = np.arange(total)
    d = history_weights(total)
    lag = n[:, None] - n[None, :]
    hist = np.where(lag >= 0, d[np.maximum(lag, 0)], 0.0)
    first = np.where(n < half, d, 0.0)
    angle = 2.0 * math.pi * ((n[:, None] * n[None, :]) % total) / total
    lam = (first[None, :] * np.exp(-1j * angle)).sum(1)
    fwd = np.zeros((owners, 2, here, total))
    inv = np.zeros((total, owners, 2, here))
    lams = np.zeros((owners, 2, 2, here))
    for q in range(owners):
        for j in range(here):
            k = q * here + j
            if k == 0:
                fwd[q, 0, j] = 1.0
                fwd[q, 1, j] = np.cos(angle[half])
                inv[:, q, 0, j] = 1.0 / total
                inv[:, q, 1, j] = np.cos(angle[half]) / total
                lams[q, 0, :, j] = lam[0].real, lam[half].real
            else:
                fwd[q, 0, j] = np.cos(angle[k])
                fwd[q, 1, j] = -np.sin(angle[k])
                inv[:, q, 0, j] = 2.0 * np.cos(angle[k]) / total
                inv[:, q, 1, j] = -2.0 * np.sin(angle[k]) / total
                lams[q, 0, :, j] = lam[k].real
                lams[q, 1, :, j] = lam[k].imag
    fwd = fwd.reshape(total, total)
    first_mat = np.zeros((2 * total, total, 2))
    spectra = first_mat.reshape(owners, 2, 2 * here, total, 2)
    spectra[:, 0, :, :, 0] = (-fwd @ hist).reshape(owners, 2 * here, total)
    spectra[:, 0, :, :, 1] = fwd.reshape(owners, 2 * here, total)
    spectra[:, 1, :, :, 0] = fwd.reshape(owners, 2 * here, total)
    flat = inv.reshape(total, owners, 2 * here)
    second_mat = np.zeros((3, total, owners, 3, 2 * here))
    second_mat[0, :, :, 0] = flat
    second_mat[1, :, :, 0] = (hist @ inv.reshape(total, total)).reshape(flat.shape)
    second_mat[1, :, :, 1] = flat
    second_mat[2, :, :, 2] = flat
    second_mat = second_mat.reshape(3, total // own, own, 3 * total).transpose(2, 0, 1, 3)
    f32 = np.float32
    return (
        first_mat.reshape(2 * total, 2 * total).astype(f32),
        second_mat.reshape(3 * total, 3 * total).astype(f32),
        lams.reshape(owners, 2, 2 * here).astype(f32),
    )


def local_call(kernel, outs, inputs, scratch=(), keep_in=True, keep_out=True):
    vmem = pl.BlockSpec(memory_space=pltpu.VMEM)
    made = pltpu.VMEM if keep_out else jax.ShapeDtypeStruct
    call = pl.pallas_call(
        kernel,
        out_shape=[made(shape, jnp.float32) for shape in outs],
        in_specs=[vmem] * inputs,
        out_specs=[vmem] * len(outs),
        scratch_shapes=list(scratch),
    )

    def placed(*args):
        if keep_in:
            args = [pltpu.with_memory_space_constraint(a, pltpu.VMEM) for a in args]
        return call(*args)

    return placed


def iota(shape, dim):
    return lax.broadcasted_iota(jnp.int32, shape, dim)


def make_entry(nz, ny, nx):
    lanes = nz * ny

    def kernel(u, f, kappa, out, s):
        row, lane = iota((ny, nx), 0), iota((ny, nx), 1)
        for z in range(nz):
            v = u[z]
            near = jnp.where(row == 0, 0.0, pltpu.roll(v, 1, 0))
            near = near + jnp.where(row == ny - 1, 0.0, pltpu.roll(v, ny - 1, 0))
            near = near + jnp.where(lane == 0, 0.0, pltpu.roll(v, 1, 1))
            near = near + jnp.where(lane == nx - 1, 0.0, pltpu.roll(v, nx - 1, 1))
            if z > 0:
                near = near + u[z - 1]
            if z < nz - 1:
                near = near + u[z + 1]
            s[z] = f[z] - kappa[z] * (6.0 * v - near)
        out[pl.ds(0, nx, stride=2), :] = u[...].reshape(lanes, nx).T
        out[pl.ds(1, nx, stride=2), :] = s[...].reshape(lanes, nx).T

    scratch = [pltpu.VMEM((nz, ny, nx), jnp.float32)]
    return local_call(kernel, [(2 * nx, lanes)], 3, scratch, keep_in=False)


def make_forward(total, lanes):
    def kernel(mat, cells, spec):
        spec[...] = jnp.dot(
            mat[...], cells[...], precision=HIGH, preferred_element_type=jnp.float32
        )

    return local_call(kernel, [(2 * total, lanes)], 2)


def make_border(own, depth, rows, lanes, ny):
    def kernel(spec, kap, out, to_right, to_left):
        lane = iota((rows, lanes), 1)
        first, last = lane < ny, lane >= lanes - ny
        for c in range(own):
            for h in range(2):
                at = 2 * (depth + c) + h
                k = jnp.broadcast_to(kap[at : at + 1, :], (rows, lanes))
                other = pltpu.roll(spec[c, 1 - h, rows:, :], ny if h else lanes - ny, 1)
                value = spec[c, h, :rows, :] + jnp.where(first if h else last, k * other, 0.0)
                out[c, h] = value
                if c >= own - depth:
                    to_right[c - (own - depth), h] = value
                if c < depth:
                    to_left[c, h] = value

    shapes = [(count, 2, rows, lanes) for count in (own, depth, depth)]
    return local_call(kernel, shapes, 2)


def make_backward(total, own, lanes):
    blocks = total // own
    pad = 3 * blocks + 8

    def kernel(mat, back, out):
        fields = jnp.concatenate(
            [back[:, 3 * h : 3 * h + 3].reshape(3 * total, lanes) for h in range(2)], axis=1
        )
        every = jnp.dot(mat[...], fields, precision=HIGH, preferred_element_type=jnp.float32)
        ri = ii = 0.0
        for c in range(own):
            at = 3 * blocks * c
            image = every[at + blocks : at + 2 * blocks]
            ri = ri + every[at + 2 * blocks : at + 3 * blocks] * image
            ii = ii + image * image
            out[pad * c : pad * c + 3 * blocks, :] = every[at : at + 3 * blocks, :lanes]
        ri = jnp.sum(ri[:, :lanes] + ri[:, lanes:], axis=0, keepdims=True)
        ii = jnp.sum(ii[:, :lanes] + ii[:, lanes:], axis=0, keepdims=True)
        low = iota((1, lanes), 1) < lanes // 2
        sums = jnp.where(low, ri + pltpu.roll(ri, lanes // 2, 1), ii + pltpu.roll(ii, lanes // 2, 1))
        for c in range(own):
            out[pad * c + 3 * blocks : pad * (c + 1), :] = jnp.broadcast_to(sums, (8, lanes))

    return local_call(kernel, [(own * pad, lanes)], 2)


def make_turn(blocks, own, lanes):
    pad, rows = 3 * blocks + 8, 3 * own + 1

    def kernel(near, out):
        sums = 0.0
        for c in range(own):
            for k in range(3):
                at = pad * c + blocks * k
                out[pl.ds(own * k + c, blocks, stride=rows), :] = near[at : at + blocks, :]
            sums = sums + near[pad * c + 3 * blocks : pad * c + 3 * blocks + 1, :]
        out[pl.ds(3 * own, blocks, stride=rows), :] = jnp.broadcast_to(sums, (blocks, lanes))

    return local_call(kernel, [(blocks * rows, lanes)], 1)


def make_exit(nz, ny, nx, blocks, own):
    lanes = nz * ny
    rows = 3 * own + 1

    def kernel(times, u, new_u, new_r):
        low = iota((1, lanes), 1) < lanes // 2
        row = jnp.sum(times[pl.ds(3 * own, blocks, stride=rows), :], axis=0, keepdims=True)
        ri = jnp.sum(jnp.where(low, row, 0.0), axis=1, keepdims=True)
        ii = jnp.sum(jnp.where(low, 0.0, row), axis=1, keepdims=True)
        step = (ri / ii).reshape(1, 1, 1)

        def slab(k):
            parts = [times[rows * b + own * k : rows * b + own * (k + 1), :] for b in range(blocks)]
            return jnp.concatenate(parts, axis=0).T.reshape(nz, ny, nx)

        new_u[...] = u[...] + step * slab(0)
        new_r[...] = slab(2) - step * slab(1)

    return local_call(kernel, [(nz, ny, nx)] * 2, 2, keep_out=False)


def make_sweeps(own, depth, rows, lanes, ny):
    cols = own + 2 * depth
    shape = (rows, lanes)

    def kernel(left, mid, right, kap, lam, out, start, same, cross, ping, pong):
        flat = [(ref, c) for ref in (left, mid, right) for c in range(ref.shape[0])]
        lane = iota(shape, 1)
        y = lane % ny
        y_first, y_last = y == 0, y == ny - 1
        z_first, z_last = lane < ny, lane >= lanes - ny
        sign = jnp.where(iota(shape, 0) < rows // 2, -1.0, 1.0)
        lam_r, lam_i = lam[0], lam[1]
        lam_ii = lam_i * lam_i

        def swap(v):
            return pltpu.roll(v, rows // 2, 0)

        for c in range(cols):
            ref, at = flat[c]
            for h in range(2):
                k = jnp.broadcast_to(kap[2 * c + h : 2 * c + h + 1, :], shape)
                diag = lam_r + 6.0 * k
                over = 1.0 / (diag * diag + lam_ii)
                g = diag * over
                g_cross = sign * (-lam_i * over)
                spec = ref[at, h]
                first = g * spec + g_cross * swap(spec)
                start[c, h] = first
                ping[c, h] = first
                same[c, h] = g * k
                cross[c, h] = g_cross * k

        def around(buf, c):
            a, b = buf[c, 0], buf[c, 1]
            down_a, down_b = pltpu.roll(a, ny, 1), pltpu.roll(b, ny, 1)
            up_a, up_b = pltpu.roll(a, lanes - ny, 1), pltpu.roll(b, lanes - ny, 1)

            def along_y(v):
                return jnp.where(y_first, 0.0, pltpu.roll(v, 1, 1)) + jnp.where(
                    y_last, 0.0, pltpu.roll(v, lanes - 1, 1)
                )

            na = jnp.where(z_first, 0.0, down_a) + jnp.where(z_last, up_b, up_a) + along_y(a)
            nb = jnp.where(z_first, down_a, down_b) + jnp.where(z_last, 0.0, up_b) + along_y(b)
            return (
                na + buf[c - 1, 0] + buf[c + 1, 0],
                nb + buf[c - 1, 1] + buf[c + 1, 1],
            )

        now, then = ping, pong
        for sweep in range(1, SWEEPS):
            for c in range(sweep, cols - sweep):
                near = around(now, c)
                for h in range(2):
                    n = near[h]
                    then[c, h] = start[c, h] + (same[c, h] * n + cross[c, h] * swap(n))
            now, then = then, now
        for c in range(depth, depth + own):
            near = around(now, c)
            for h in range(2):
                sol = now[c, h]
                k = jnp.broadcast_to(kap[2 * c + h : 2 * c + h + 1, :], shape)
                stiff = k * (6.0 * sol - near[h])
                for core in range(2):
                    row, at = 2 * (c - depth) + core, 0 if core == h else 3
                    out[row, at] = sol
                    out[row, at + 1] = stiff
                    out[row, at + 2] = mid[c - depth, h]

    field = pltpu.VMEM((cols, 2, rows, lanes), jnp.float32)
    return local_call(kernel, [(2 * own, 6, rows, lanes)], 5, [field] * 5)


def on_device(iterate, source, diffusivity):
    _, nz, ny, nx = iterate.shape
    lanes = nz * ny
    blocks, pair = lax.axis_size("blocks"), lax.axis_size("pair")
    own = pair * lax.axis_size("tm_1")
    cores = lax.axis_size("space")
    total = blocks * own
    owners = own * cores
    rows = total // owners
    depth = SWEEPS
    first_mat, second_mat, lams = tables(total, owners, own)
    core = lax.axis_index("space")
    block = lax.axis_index("blocks")
    swap = [(0, 1), (1, 0)]

    u, f = iterate[0], source[0]
    (send,) = make_entry(nz, ny, nx)(u, f, diffusivity)
    send, diffusivity = lax.optimization_barrier((send, diffusivity))
    cells = lax.all_to_all(
        send.reshape(total, 2, lanes), TM, split_axis=0, concat_axis=0, tiled=True
    ).reshape(2 * total, lanes)

    kap = jnp.pad(diffusivity.reshape(lanes, nx).T, ((depth, depth), (0, 0)))
    kap = lax.dynamic_slice_in_dim(kap, block * own, own + 2 * depth, axis=0)
    kap_other = lax.ppermute(kap, "space", swap)
    kap = jnp.where(
        core == 0, jnp.stack([kap, kap_other], axis=1), jnp.stack([kap_other, kap], axis=1)
    ).reshape(-1, lanes)
    lam = lax.dynamic_index_in_dim(jnp.asarray(lams), lax.axis_index(ROW), axis=0, keepdims=False)
    lam = jnp.broadcast_to(lam[:, :, None], (2, rows, lanes))
    cells, kap, lam = lax.optimization_barrier((cells, kap, lam))

    (spec,) = make_forward(total, lanes)(first_mat, cells)
    spec = lax.all_to_all(
        spec.reshape(owners, 2 * rows, lanes), ROW, split_axis=0, concat_axis=0, tiled=True
    )
    spec, to_right, to_left = make_border(own, depth, rows, lanes, ny)(
        spec.reshape(own, cores, 2 * rows, lanes), kap
    )

    def shifted(value, offset):
        pairs = [(i, i + offset) for i in range(blocks) if 0 <= i + offset < blocks]
        return lax.ppermute(value, "blocks", pairs)

    left = shifted(to_right, 1)
    right = shifted(to_left, -1)
    (back,) = make_sweeps(own, depth, rows, lanes, ny)(left, spec, right, kap, lam)
    back = lax.all_to_all(back, ROW, split_axis=0, concat_axis=0, tiled=True)
    (near,) = make_backward(total, own, lanes)(second_mat, back)
    near = lax.all_to_all(
        near.reshape(own, -1, lanes), TM[1:], split_axis=0, concat_axis=0, tiled=True
    )
    (far,) = make_turn(blocks, own, lanes)(near.reshape(-1, lanes))
    times = lax.all_to_all(
        far.reshape(blocks, 3 * own + 1, 1, lanes), "blocks", split_axis=0, concat_axis=0, tiled=True
    )
    new_iterate, new_residual = make_exit(nz, ny, nx, blocks, own)(times.reshape(-1, lanes), u)
    return (new_iterate[None], new_residual[None])


def solution(mesh):
    split = Mesh(
        mesh.devices.reshape(mesh.shape["groups"], 16, 2, 4, mesh.shape["space"]),
        ("groups", "blocks", "pair", "tm_1", "space"),
    )
    placed = (
        P(GROUPS_TM, "space", None, None),
        P(GROUPS_TM, "space", None, None),
        P(("groups", "space"), None, None),
    )
    return jax.shard_map(
        on_device,
        mesh=split,
        in_specs=placed,
        out_specs=(P(GROUPS_TM, "space", None, None), P(GROUPS_TM, "space", None, None)),
        check_vma=False,
    )
```

```python
import math

import jax
import jax.numpy as jnp
import numpy as np
from jax import lax
from jax.experimental import pallas as pl
from jax.experimental.pallas import tpu as pltpu
from jax.sharding import Mesh
from jax.sharding import PartitionSpec as P

SWEEPS = 6
TM = ("blocks", "pair", "tm_1")
ROW = ("pair", "tm_1", "space")
GROUPS_TM = ("groups", "blocks", "pair", "tm_1")
HIGH = lax.Precision.HIGHEST

frac_order = 0.3
step_length = 0.01
gamma_factor = 0.9086387328532904


def history_weights(count):
    k = np.arange(count + 1, dtype=np.float64) ** (1.0 - frac_order)
    b = k[1:] - k[:-1]
    d = np.concatenate([[1.0], b[1:] - b[:-1]])
    return d / (step_length**frac_order * gamma_factor)


def tables(total, owners, own):
    half = total // 2
    here = half // owners
    n = np.arange(total)
    d = history_weights(total)
    lag = n[:, None] - n[None, :]
    hist = np.where(lag >= 0, d[np.maximum(lag, 0)], 0.0)
    first = np.where(n < half, d, 0.0)
    angle = 2.0 * math.pi * ((n[:, None] * n[None, :]) % total) / total
    lam = (first[None, :] * np.exp(-1j * angle)).sum(1)
    fwd = np.zeros((owners, 2, here, total))
    inv = np.zeros((total, owners, 2, here))
    lams = np.zeros((owners, 2, 2, here))
    for q in range(owners):
        for j in range(here):
            k = q * here + j
            if k == 0:
                fwd[q, 0, j] = 1.0
                fwd[q, 1, j] = np.cos(angle[half])
                inv[:, q, 0, j] = 1.0 / total
                inv[:, q, 1, j] = np.cos(angle[half]) / total
                lams[q, 0, :, j] = lam[0].real, lam[half].real
            else:
                fwd[q, 0, j] = np.cos(angle[k])
                fwd[q, 1, j] = -np.sin(angle[k])
                inv[:, q, 0, j] = 2.0 * np.cos(angle[k]) / total
                inv[:, q, 1, j] = -2.0 * np.sin(angle[k]) / total
                lams[q, 0, :, j] = lam[k].real
                lams[q, 1, :, j] = lam[k].imag
    fwd = fwd.reshape(total, total)
    first_mat = np.zeros((2 * total, total, 2))
    spectra = first_mat.reshape(owners, 2, 2 * here, total, 2)
    spectra[:, 0, :, :, 0] = (-fwd @ hist).reshape(owners, 2 * here, total)
    spectra[:, 0, :, :, 1] = fwd.reshape(owners, 2 * here, total)
    spectra[:, 1, :, :, 0] = fwd.reshape(owners, 2 * here, total)
    flat = inv.reshape(total, owners, 2 * here)
    second_mat = np.zeros((3, total, owners, 3, 2 * here))
    second_mat[0, :, :, 0] = flat
    second_mat[1, :, :, 0] = (hist @ inv.reshape(total, total)).reshape(flat.shape)
    second_mat[1, :, :, 1] = flat
    second_mat[2, :, :, 2] = flat
    second_mat = second_mat.reshape(3, total // own, own, 3 * total).transpose(2, 0, 1, 3)
    f32 = np.float32
    return (
        first_mat.reshape(2 * total, 2 * total).astype(f32),
        second_mat.reshape(3 * total, 3 * total).astype(f32),
        lams.reshape(owners, 2, 2 * here).astype(f32),
    )


def local_call(kernel, name, outs, inputs, scratch=(), keep_in=True, keep_out=True):
    vmem = pl.BlockSpec(memory_space=pltpu.VMEM)
    made = pltpu.VMEM if keep_out else jax.ShapeDtypeStruct
    call = pl.pallas_call(
        kernel,
        out_shape=[made(shape, jnp.float32) for shape in outs],
        in_specs=[vmem] * inputs,
        out_specs=[vmem] * len(outs),
        scratch_shapes=list(scratch),
        name=name,
    )

    def placed(*args):
        if keep_in:
            args = [pltpu.with_memory_space_constraint(a, pltpu.VMEM) for a in args]
        return call(*args)

    return placed


def iota(shape, dim):
    return lax.broadcasted_iota(jnp.int32, shape, dim)


def make_entry(nz, ny, nx):
    lanes = nz * ny

    def kernel(u, f, kappa, out, s):
        row, lane = iota((ny, nx), 0), iota((ny, nx), 1)
        for z in range(nz):
            v = u[z]
            near = jnp.where(row == 0, 0.0, pltpu.roll(v, 1, 0))
            near = near + jnp.where(row == ny - 1, 0.0, pltpu.roll(v, ny - 1, 0))
            near = near + jnp.where(lane == 0, 0.0, pltpu.roll(v, 1, 1))
            near = near + jnp.where(lane == nx - 1, 0.0, pltpu.roll(v, nx - 1, 1))
            if z > 0:
                near = near + u[z - 1]
            if z < nz - 1:
                near = near + u[z + 1]
            s[z] = f[z] - kappa[z] * (6.0 * v - near)
        out[pl.ds(0, nx, stride=2), :] = u[...].reshape(lanes, nx).T
        out[pl.ds(1, nx, stride=2), :] = s[...].reshape(lanes, nx).T

    scratch = [pltpu.VMEM((nz, ny, nx), jnp.float32)]
    return local_call(kernel, "entry", [(2 * nx, lanes)], 3, scratch, keep_in=False)


def make_forward(total, owners, lanes, ny):
    rows = total // owners

    def kernel(mat, cells, info, out, both):
        both[...] = jnp.dot(
            mat[...], cells[...], precision=HIGH, preferred_element_type=jnp.float32
        )
        lane = iota((owners, lanes), 1)
        lower = info[3:4, :]
        edge = jnp.zeros((owners, lanes), jnp.float32)
        for j in range(rows):
            x = both[pl.ds(rows + j, owners, stride=2 * rows), :]
            at = ny * (rows - 1 - j)
            moved = lower * pltpu.roll(x, (at + ny) % lanes, 1) + (1.0 - lower) * (
                pltpu.roll(x, at, 1) if at else x
            )
            edge = jnp.where((lane >= at) & (lane < at + ny), moved, edge)
        for q in range(owners):
            out[12 * q : 12 * q + rows, :] = both[2 * rows * q : 2 * rows * q + rows, :]
        out[pl.ds(rows, owners, stride=12), :] = edge
        for m in range(3):
            row = jnp.broadcast_to(info[m : m + 1, :], (owners, lanes))
            out[pl.ds(rows + 1 + m, owners, stride=12), :] = row

    scratch = [pltpu.VMEM((2 * total, lanes), jnp.float32)]
    return local_call(kernel, "forward", [(12 * owners, lanes)], 3, scratch)


def make_border(own, depth, rows, lanes, ny):
    def kernel(spec, out, to_right, to_left, kap):
        lane = iota((rows, lanes), 1)
        first, last = lane < ny, lane >= lanes - ny
        for c in range(own):
            for h in range(2):
                for m in range(3):
                    if c + own * m < own + 2 * depth:
                        at = 2 * (c + own * m) + h
                        line = 12 * (2 * c + h) + rows + 1 + m
                        kap[at : at + 1, :] = spec[line : line + 1, :]
        for c in range(own):
            for h in range(2):
                at = 2 * (depth + c) + h
                k = jnp.broadcast_to(kap[at : at + 1, :], (rows, lanes))
                line = 12 * (2 * c + 1 - h) + rows
                edge = jnp.broadcast_to(spec[line : line + 1, :], (rows, lanes))
                other = pltpu.roll(edge, ny if h else 0, 1, stride=ny, stride_axis=0)
                line = 12 * (2 * c + h)
                value = spec[line : line + rows, :] + jnp.where(first if h else last, k * other, 0.0)
                out[c, h] = value
                if c >= own - depth:
                    to_right[c - (own - depth), h] = value
                if c < depth:
                    to_left[c, h] = value

    shapes = [(count, 2, rows, lanes) for count in (own, depth, depth)]
    return local_call(kernel, "border", shapes + [(2 * (own + 2 * depth), lanes)], 1)


def make_backward(total, own, lanes):
    blocks = total // own
    pad = 3 * blocks + 8

    def kernel(mat, back, out):
        fields = jnp.concatenate(
            [back[:, 3 * h : 3 * h + 3].reshape(3 * total, lanes) for h in range(2)], axis=1
        )
        every = jnp.dot(mat[...], fields, precision=HIGH, preferred_element_type=jnp.float32)
        ri = ii = 0.0
        for c in range(own):
            at = 3 * blocks * c
            image = every[at + blocks : at + 2 * blocks]
            ri = ri + every[at + 2 * blocks : at + 3 * blocks] * image
            ii = ii + image * image
            out[pad * c : pad * c + 3 * blocks, :] = every[at : at + 3 * blocks, :lanes]
        ri = jnp.sum(ri[:, :lanes] + ri[:, lanes:], axis=0, keepdims=True)
        ii = jnp.sum(ii[:, :lanes] + ii[:, lanes:], axis=0, keepdims=True)
        low = iota((1, lanes), 1) < lanes // 2
        sums = jnp.where(low, ri + pltpu.roll(ri, lanes // 2, 1), ii + pltpu.roll(ii, lanes // 2, 1))
        for c in range(own):
            out[pad * c + 3 * blocks : pad * (c + 1), :] = jnp.broadcast_to(sums, (8, lanes))

    return local_call(kernel, "backward", [(own * pad, lanes)], 2)


def make_turn(blocks, own, lanes):
    pad, rows = 3 * blocks + 8, 3 * own + 1

    def kernel(near, out):
        sums = 0.0
        for c in range(own):
            for k in range(3):
                at = pad * c + blocks * k
                out[pl.ds(own * k + c, blocks, stride=rows), :] = near[at : at + blocks, :]
            sums = sums + near[pad * c + 3 * blocks : pad * c + 3 * blocks + 1, :]
        out[pl.ds(3 * own, blocks, stride=rows), :] = jnp.broadcast_to(sums, (blocks, lanes))

    return local_call(kernel, "turn", [(blocks * rows, lanes)], 1)


def make_exit(nz, ny, nx, blocks, own):
    lanes = nz * ny
    rows = 3 * own + 1

    def kernel(times, u, new_u, new_r):
        low = iota((1, lanes), 1) < lanes // 2
        row = jnp.sum(times[pl.ds(3 * own, blocks, stride=rows), :], axis=0, keepdims=True)
        ri = jnp.sum(jnp.where(low, row, 0.0), axis=1, keepdims=True)
        ii = jnp.sum(jnp.where(low, 0.0, row), axis=1, keepdims=True)
        step = (ri / ii).reshape(1, 1, 1)

        def slab(k):
            parts = [times[rows * b + own * k : rows * b + own * (k + 1), :] for b in range(blocks)]
            return jnp.concatenate(parts, axis=0).T.reshape(nz, ny, nx)

        new_u[...] = u[...] + step * slab(0)
        new_r[...] = slab(2) - step * slab(1)

    return local_call(kernel, "exit", [(nz, ny, nx)] * 2, 2, keep_out=False)


def make_sweeps(own, depth, rows, lanes, ny):
    cols = own + 2 * depth
    shape = (rows, lanes)

    def kernel(left, mid, right, kap, lam, out, start, same, cross, ping, pong):
        flat = [(ref, c) for ref in (left, mid, right) for c in range(ref.shape[0])]
        lane = iota(shape, 1)
        y = lane % ny
        y_first, y_last = y == 0, y == ny - 1
        z_first, z_last = lane < ny, lane >= lanes - ny
        sign = jnp.where(iota(shape, 0) < rows // 2, -1.0, 1.0)
        lam_r, lam_i = lam[0], lam[1]
        lam_ii = lam_i * lam_i

        def swap(v):
            return pltpu.roll(v, rows // 2, 0)

        for c in range(cols):
            ref, at = flat[c]
            for h in range(2):
                k = jnp.broadcast_to(kap[2 * c + h : 2 * c + h + 1, :], shape)
                diag = lam_r + 6.0 * k
                over = 1.0 / (diag * diag + lam_ii)
                g = diag * over
                g_cross = sign * (-lam_i * over)
                spec = ref[at, h]
                first = g * spec + g_cross * swap(spec)
                start[c, h] = first
                ping[c, h] = first
                same[c, h] = g * k
                cross[c, h] = g_cross * k

        def around(buf, c):
            a, b = buf[c, 0], buf[c, 1]
            down_a, down_b = pltpu.roll(a, ny, 1), pltpu.roll(b, ny, 1)
            up_a, up_b = pltpu.roll(a, lanes - ny, 1), pltpu.roll(b, lanes - ny, 1)

            def along_y(v):
                return jnp.where(y_first, 0.0, pltpu.roll(v, 1, 1)) + jnp.where(
                    y_last, 0.0, pltpu.roll(v, lanes - 1, 1)
                )

            na = jnp.where(z_first, 0.0, down_a) + jnp.where(z_last, up_b, up_a) + along_y(a)
            nb = jnp.where(z_first, down_a, down_b) + jnp.where(z_last, 0.0, up_b) + along_y(b)
            return (
                na + buf[c - 1, 0] + buf[c + 1, 0],
                nb + buf[c - 1, 1] + buf[c + 1, 1],
            )

        now, then = ping, pong
        for sweep in range(1, SWEEPS):
            for c in range(sweep, cols - sweep):
                near = around(now, c)
                for h in range(2):
                    n = near[h]
                    then[c, h] = start[c, h] + (same[c, h] * n + cross[c, h] * swap(n))
            now, then = then, now
        for c in range(depth, depth + own):
            near = around(now, c)
            for h in range(2):
                sol = now[c, h]
                k = jnp.broadcast_to(kap[2 * c + h : 2 * c + h + 1, :], shape)
                stiff = k * (6.0 * sol - near[h])
                for core in range(2):
                    row, at = 2 * (c - depth) + core, 0 if core == h else 3
                    out[row, at] = sol
                    out[row, at + 1] = stiff
                    out[row, at + 2] = mid[c - depth, h]

    field = pltpu.VMEM((cols, 2, rows, lanes), jnp.float32)
    return local_call(kernel, "sweeps", [(2 * own, 6, rows, lanes)], 5, [field] * 5)


def on_device(iterate, source, diffusivity):
    _, nz, ny, nx = iterate.shape
    lanes = nz * ny
    blocks, pair = lax.axis_size("blocks"), lax.axis_size("pair")
    own = pair * lax.axis_size("tm_1")
    cores = lax.axis_size("space")
    total = blocks * own
    owners = own * cores
    rows = total // owners
    depth = SWEEPS
    first_mat, second_mat, lams = tables(total, owners, own)
    core = lax.axis_index("space")
    block = lax.axis_index("blocks")

    u, f = iterate[0], source[0]
    (send,) = make_entry(nz, ny, nx)(u, f, diffusivity)
    start = block * own + lax.axis_index(TM[1:])
    owner = lax.axis_index(ROW)
    lower = jnp.where(core == 0, 1.0, 0.0)
    send, start, owner, lower = lax.optimization_barrier((send, start, owner, lower))
    cells = lax.all_to_all(
        send.reshape(total, 2, lanes), TM, split_axis=0, concat_axis=0, tiled=True
    ).reshape(2 * total, lanes)

    cells, kappa, start, lower = lax.optimization_barrier((cells, diffusivity, start, lower))
    columns = jnp.pad(kappa.reshape(lanes, nx).T, ((depth, 2 * own), (0, 0)))
    columns = lax.dynamic_slice_in_dim(columns, start, 2 * own + 1, axis=0)
    lower = jnp.broadcast_to(lower, (1, lanes))
    info = jnp.concatenate([columns[0:1], columns[own : own + 1], columns[2 * own :], lower], axis=0)
    (spec,) = make_forward(total, owners, lanes, ny)(first_mat, cells, info)
    spec = lax.all_to_all(
        spec.reshape(owners, 12, 1, lanes), ROW, split_axis=0, concat_axis=0, tiled=True
    )
    spec, to_right, to_left, kap = make_border(own, depth, rows, lanes, ny)(spec.reshape(-1, lanes))
    to_right, to_left, lams, owner = lax.optimization_barrier(
        (to_right, to_left, jnp.asarray(lams), owner)
    )
    lam = lax.dynamic_index_in_dim(lams, owner, axis=0, keepdims=False)
    lam = jnp.broadcast_to(lam[:, :, None], (2, rows, lanes))

    def shifted(value, offset):
        pairs = [(i, i + offset) for i in range(blocks) if 0 <= i + offset < blocks]
        return lax.ppermute(value, "blocks", pairs)

    left = shifted(to_right, 1)
    right = shifted(to_left, -1)
    (back,) = make_sweeps(own, depth, rows, lanes, ny)(left, spec, right, kap, lam)
    back = lax.all_to_all(back, ROW, split_axis=0, concat_axis=0, tiled=True)
    (near,) = make_backward(total, own, lanes)(second_mat, back)
    near = lax.all_to_all(
        near.reshape(own, -1, lanes), TM[1:], split_axis=0, concat_axis=0, tiled=True
    )
    (far,) = make_turn(blocks, own, lanes)(near.reshape(-1, lanes))
    times = lax.all_to_all(
        far.reshape(blocks, 3 * own + 1, 1, lanes), "blocks", split_axis=0, concat_axis=0, tiled=True
    )
    new_iterate, new_residual = make_exit(nz, ny, nx, blocks, own)(times.reshape(-1, lanes), u)
    return (new_iterate[None], new_residual[None])


def solution(mesh):
    split = Mesh(
        mesh.devices.reshape(mesh.shape["groups"], 16, 2, 4, mesh.shape["space"]),
        ("groups", "blocks", "pair", "tm_1", "space"),
    )
    placed = (
        P(GROUPS_TM, "space", None, None),
        P(GROUPS_TM, "space", None, None),
        P(("groups", "space"), None, None),
    )
    return jax.shard_map(
        on_device,
        mesh=split,
        in_specs=placed,
        out_specs=(P(GROUPS_TM, "space", None, None), P(GROUPS_TM, "space", None, None)),
        check_vma=False,
    )
```

```python
import math

import jax
import jax.numpy as jnp
import numpy as np
from jax import lax
from jax.experimental import pallas as pl
from jax.experimental.pallas import tpu as pltpu
from jax.sharding import Mesh
from jax.sharding import PartitionSpec as P

SWEEPS = 6
TM = ("blocks", "pair", "tm_1")
ROW = ("pair", "tm_1", "space")
GROUPS_TM = ("groups", "blocks", "pair", "tm_1")
HIGH = lax.Precision.HIGHEST

frac_order = 0.3
step_length = 0.01
gamma_factor = 0.9086387328532904


def history_weights(count):
    k = np.arange(count + 1, dtype=np.float64) ** (1.0 - frac_order)
    b = k[1:] - k[:-1]
    d = np.concatenate([[1.0], b[1:] - b[:-1]])
    return d / (step_length**frac_order * gamma_factor)


def tables(total, owners, own):
    half = total // 2
    here = half // owners
    n = np.arange(total)
    d = history_weights(total)
    lag = n[:, None] - n[None, :]
    hist = np.where(lag >= 0, d[np.maximum(lag, 0)], 0.0)
    first = np.where(n < half, d, 0.0)
    angle = 2.0 * math.pi * ((n[:, None] * n[None, :]) % total) / total
    lam = (first[None, :] * np.exp(-1j * angle)).sum(1)
    fwd = np.zeros((owners, 2, here, total))
    inv = np.zeros((total, owners, 2, here))
    lams = np.zeros((owners, 2, 2, here))
    for q in range(owners):
        for j in range(here):
            k = q * here + j
            if k == 0:
                fwd[q, 0, j] = 1.0
                fwd[q, 1, j] = np.cos(angle[half])
                inv[:, q, 0, j] = 1.0 / total
                inv[:, q, 1, j] = np.cos(angle[half]) / total
                lams[q, 0, :, j] = lam[0].real, lam[half].real
            else:
                fwd[q, 0, j] = np.cos(angle[k])
                fwd[q, 1, j] = -np.sin(angle[k])
                inv[:, q, 0, j] = 2.0 * np.cos(angle[k]) / total
                inv[:, q, 1, j] = -2.0 * np.sin(angle[k]) / total
                lams[q, 0, :, j] = lam[k].real
                lams[q, 1, :, j] = lam[k].imag
    fwd = fwd.reshape(total, total)
    first_mat = np.zeros((2 * total, total, 2))
    spectra = first_mat.reshape(owners, 2, 2 * here, total, 2)
    spectra[:, 0, :, :, 0] = (-fwd @ hist).reshape(owners, 2 * here, total)
    spectra[:, 0, :, :, 1] = fwd.reshape(owners, 2 * here, total)
    spectra[:, 1, :, :, 0] = fwd.reshape(owners, 2 * here, total)
    flat = inv.reshape(total, total)
    second_mat = np.stack([hist @ flat, flat]).reshape(2, total // own, own, total)
    second_mat = second_mat.transpose(0, 2, 1, 3)
    f32 = np.float32
    return (
        first_mat.reshape(2 * total, 2 * total).astype(f32),
        second_mat.reshape(2 * total, total).astype(f32),
        lams.reshape(owners, 2, 2 * here).astype(f32),
    )


def local_call(kernel, name, outs, inputs, scratch=(), keep_in=True, keep_out=True):
    vmem = pl.BlockSpec(memory_space=pltpu.VMEM)
    made = pltpu.VMEM if keep_out else jax.ShapeDtypeStruct
    call = pl.pallas_call(
        kernel,
        out_shape=[made(shape, jnp.float32) for shape in outs],
        in_specs=[vmem] * inputs,
        out_specs=[vmem] * len(outs),
        scratch_shapes=list(scratch),
        name=name,
    )

    def placed(*args):
        if keep_in:
            args = [pltpu.with_memory_space_constraint(a, pltpu.VMEM) for a in args]
        return call(*args)

    return placed


def iota(shape, dim):
    return lax.broadcasted_iota(jnp.int32, shape, dim)


def make_entry(nz, ny, nx):
    lanes = nz * ny

    def kernel(u, f, kappa, out, s):
        row, lane = iota((ny, nx), 0), iota((ny, nx), 1)
        for z in range(nz):
            v = u[z]
            near = jnp.where(row == 0, 0.0, pltpu.roll(v, 1, 0))
            near = near + jnp.where(row == ny - 1, 0.0, pltpu.roll(v, ny - 1, 0))
            near = near + jnp.where(lane == 0, 0.0, pltpu.roll(v, 1, 1))
            near = near + jnp.where(lane == nx - 1, 0.0, pltpu.roll(v, nx - 1, 1))
            if z > 0:
                near = near + u[z - 1]
            if z < nz - 1:
                near = near + u[z + 1]
            s[z] = f[z] - kappa[z] * (6.0 * v - near)
        out[pl.ds(0, nx, stride=2), :] = u[...].reshape(lanes, nx).T
        out[pl.ds(1, nx, stride=2), :] = s[...].reshape(lanes, nx).T

    scratch = [pltpu.VMEM((nz, ny, nx), jnp.float32)]
    return local_call(kernel, "entry", [(2 * nx, lanes)], 3, scratch, keep_in=False)


def make_forward(total, owners, lanes, ny):
    rows = total // owners

    def kernel(mat, cells, info, out, both):
        both[...] = jnp.dot(
            mat[...], cells[...], precision=HIGH, preferred_element_type=jnp.float32
        )
        lane = iota((owners, lanes), 1)
        lower = info[3:4, :]
        edge = jnp.zeros((owners, lanes), jnp.float32)
        for j in range(rows):
            x = both[pl.ds(rows + j, owners, stride=2 * rows), :]
            at = ny * (rows - 1 - j)
            moved = lower * pltpu.roll(x, (at + ny) % lanes, 1) + (1.0 - lower) * (
                pltpu.roll(x, at, 1) if at else x
            )
            edge = jnp.where((lane >= at) & (lane < at + ny), moved, edge)
        for q in range(owners):
            out[12 * q : 12 * q + rows, :] = both[2 * rows * q : 2 * rows * q + rows, :]
        out[pl.ds(rows, owners, stride=12), :] = edge
        for m in range(3):
            row = jnp.broadcast_to(info[m : m + 1, :], (owners, lanes))
            out[pl.ds(rows + 1 + m, owners, stride=12), :] = row

    scratch = [pltpu.VMEM((2 * total, lanes), jnp.float32)]
    return local_call(kernel, "forward", [(12 * owners, lanes)], 3, scratch)


def make_border(own, depth, rows, lanes, ny):
    def kernel(spec, out, to_right, to_left, kap):
        lane = iota((rows, lanes), 1)
        first, last = lane < ny, lane >= lanes - ny
        for c in range(own):
            for h in range(2):
                for m in range(3):
                    if c + own * m < own + 2 * depth:
                        at = 2 * (c + own * m) + h
                        line = 12 * (2 * c + h) + rows + 1 + m
                        kap[at : at + 1, :] = spec[line : line + 1, :]
        for c in range(own):
            for h in range(2):
                at = 2 * (depth + c) + h
                k = jnp.broadcast_to(kap[at : at + 1, :], (rows, lanes))
                line = 12 * (2 * c + 1 - h) + rows
                edge = jnp.broadcast_to(spec[line : line + 1, :], (rows, lanes))
                other = pltpu.roll(edge, ny if h else 0, 1, stride=ny, stride_axis=0)
                line = 12 * (2 * c + h)
                value = spec[line : line + rows, :] + jnp.where(first if h else last, k * other, 0.0)
                out[c, h] = value
                if c >= own - depth:
                    to_right[c - (own - depth), h] = value
                if c < depth:
                    to_left[c, h] = value

    shapes = [(count, 2, rows, lanes) for count in (own, depth, depth)]
    return local_call(kernel, "border", shapes + [(2 * (own + 2 * depth), lanes)], 1)


def make_backward(total, own, lanes):
    blocks = total // own
    pad = 3 * blocks + 8

    def kernel(mat, back, out):
        def fields(k):
            return jnp.concatenate([back[:, 3 * h + k].reshape(total, lanes) for h in range(2)], 1)

        def product(m, x):
            return jnp.dot(m, x, precision=HIGH, preferred_element_type=jnp.float32)

        first = product(mat[...], fields(0))
        rest = product(mat[total:, :], jnp.concatenate([fields(1), fields(2)], axis=1))
        correction = first[total:]
        image = first[:total] + rest[:, : 2 * lanes]
        residual = rest[:, 2 * lanes :]
        ri, ii = residual * image, image * image
        for c in range(own):
            for k, field in enumerate((correction, image, residual)):
                at = pad * c + blocks * k
                out[at : at + blocks, :] = field[blocks * c : blocks * (c + 1), :lanes]
        ri = jnp.sum(ri[:, :lanes] + ri[:, lanes:], axis=0, keepdims=True)
        ii = jnp.sum(ii[:, :lanes] + ii[:, lanes:], axis=0, keepdims=True)
        low = iota((1, lanes), 1) < lanes // 2
        sums = jnp.where(low, ri + pltpu.roll(ri, lanes // 2, 1), ii + pltpu.roll(ii, lanes // 2, 1))
        for c in range(own):
            out[pad * c + 3 * blocks : pad * (c + 1), :] = jnp.broadcast_to(sums, (8, lanes))

    return local_call(kernel, "backward", [(own * pad, lanes)], 2)


def make_turn(blocks, own, lanes):
    pad, rows = 3 * blocks + 8, 3 * own + 1

    def kernel(near, out):
        sums = 0.0
        for c in range(own):
            for k in range(3):
                at = pad * c + blocks * k
                out[pl.ds(own * k + c, blocks, stride=rows), :] = near[at : at + blocks, :]
            sums = sums + near[pad * c + 3 * blocks : pad * c + 3 * blocks + 1, :]
        out[pl.ds(3 * own, blocks, stride=rows), :] = jnp.broadcast_to(sums, (blocks, lanes))

    return local_call(kernel, "turn", [(blocks * rows, lanes)], 1)


def make_exit(nz, ny, nx, blocks, own):
    lanes = nz * ny
    rows = 3 * own + 1

    def kernel(times, u, new_u, new_r):
        low = iota((1, lanes), 1) < lanes // 2
        row = jnp.sum(times[pl.ds(3 * own, blocks, stride=rows), :], axis=0, keepdims=True)
        ri = jnp.sum(jnp.where(low, row, 0.0), axis=1, keepdims=True)
        ii = jnp.sum(jnp.where(low, 0.0, row), axis=1, keepdims=True)
        step = (ri / ii).reshape(1, 1, 1)

        def slab(k):
            parts = [times[rows * b + own * k : rows * b + own * (k + 1), :] for b in range(blocks)]
            return jnp.concatenate(parts, axis=0).T.reshape(nz, ny, nx)

        new_u[...] = u[...] + step * slab(0)
        new_r[...] = slab(2) - step * slab(1)

    return local_call(kernel, "exit", [(nz, ny, nx)] * 2, 2, keep_out=False)


def make_sweeps(own, depth, rows, lanes, ny):
    cols = own + 2 * depth
    shape = (rows, lanes)

    def kernel(left, mid, right, kap, lam, out, start, same, cross, ping, pong):
        flat = [(ref, c) for ref in (left, mid, right) for c in range(ref.shape[0])]
        lane = iota(shape, 1)
        y = lane % ny
        y_first, y_last = y == 0, y == ny - 1
        z_first, z_last = lane < ny, lane >= lanes - ny
        sign = jnp.where(iota(shape, 0) < rows // 2, -1.0, 1.0)
        lam_r, lam_i = lam[0], lam[1]
        lam_ii = lam_i * lam_i

        def swap(v):
            return pltpu.roll(v, rows // 2, 0)

        for c in range(cols):
            ref, at = flat[c]
            for h in range(2):
                k = jnp.broadcast_to(kap[2 * c + h : 2 * c + h + 1, :], shape)
                diag = lam_r + 6.0 * k
                over = 1.0 / (diag * diag + lam_ii)
                g = diag * over
                g_cross = sign * (-lam_i * over)
                spec = ref[at, h]
                first = g * spec + g_cross * swap(spec)
                start[c, h] = first
                ping[c, h] = first
                same[c, h] = g * k
                cross[c, h] = g_cross * k

        def around(buf, c):
            a, b = buf[c, 0], buf[c, 1]
            down_a, down_b = pltpu.roll(a, ny, 1), pltpu.roll(b, ny, 1)
            up_a, up_b = pltpu.roll(a, lanes - ny, 1), pltpu.roll(b, lanes - ny, 1)

            def along_y(v):
                return jnp.where(y_first, 0.0, pltpu.roll(v, 1, 1)) + jnp.where(
                    y_last, 0.0, pltpu.roll(v, lanes - 1, 1)
                )

            na = jnp.where(z_first, 0.0, down_a) + jnp.where(z_last, up_b, up_a) + along_y(a)
            nb = jnp.where(z_first, down_a, down_b) + jnp.where(z_last, 0.0, up_b) + along_y(b)
            return (
                na + buf[c - 1, 0] + buf[c + 1, 0],
                nb + buf[c - 1, 1] + buf[c + 1, 1],
            )

        now, then = ping, pong
        for sweep in range(1, SWEEPS):
            for c in range(sweep, cols - sweep):
                near = around(now, c)
                for h in range(2):
                    n = near[h]
                    then[c, h] = start[c, h] + (same[c, h] * n + cross[c, h] * swap(n))
            now, then = then, now
        for c in range(depth, depth + own):
            near = around(now, c)
            for h in range(2):
                sol = now[c, h]
                k = jnp.broadcast_to(kap[2 * c + h : 2 * c + h + 1, :], shape)
                stiff = k * (6.0 * sol - near[h])
                for core in range(2):
                    row, at = 2 * (c - depth) + core, 0 if core == h else 3
                    out[row, at] = sol
                    out[row, at + 1] = stiff
                    out[row, at + 2] = mid[c - depth, h]

    field = pltpu.VMEM((cols, 2, rows, lanes), jnp.float32)
    return local_call(kernel, "sweeps", [(2 * own, 6, rows, lanes)], 5, [field] * 5)


def on_device(iterate, source, diffusivity):
    _, nz, ny, nx = iterate.shape
    lanes = nz * ny
    blocks, pair = lax.axis_size("blocks"), lax.axis_size("pair")
    own = pair * lax.axis_size("tm_1")
    cores = lax.axis_size("space")
    total = blocks * own
    owners = own * cores
    rows = total // owners
    depth = SWEEPS
    first_mat, second_mat, lams = tables(total, owners, own)
    core = lax.axis_index("space")
    block = lax.axis_index("blocks")

    u, f = iterate[0], source[0]
    (send,) = make_entry(nz, ny, nx)(u, f, diffusivity)
    start = block * own + lax.axis_index(TM[1:])
    owner = lax.axis_index(ROW)
    lower = jnp.where(core == 0, 1.0, 0.0)
    send, start, owner, lower = lax.optimization_barrier((send, start, owner, lower))
    cells = lax.all_to_all(
        send.reshape(total, 2, lanes), TM, split_axis=0, concat_axis=0, tiled=True
    ).reshape(2 * total, lanes)

    cells, kappa, start, lower = lax.optimization_barrier((cells, diffusivity, start, lower))
    columns = jnp.pad(kappa.reshape(lanes, nx).T, ((depth, 2 * own), (0, 0)))
    columns = lax.dynamic_slice_in_dim(columns, start, 2 * own + 1, axis=0)
    lower = jnp.broadcast_to(lower, (1, lanes))
    info = jnp.concatenate([columns[0:1], columns[own : own + 1], columns[2 * own :], lower], axis=0)
    (spec,) = make_forward(total, owners, lanes, ny)(first_mat, cells, info)
    spec = lax.all_to_all(
        spec.reshape(owners, 12, 1, lanes), ROW, split_axis=0, concat_axis=0, tiled=True
    )
    spec, to_right, to_left, kap = make_border(own, depth, rows, lanes, ny)(spec.reshape(-1, lanes))
    to_right, to_left, lams, owner = lax.optimization_barrier(
        (to_right, to_left, jnp.asarray(lams), owner)
    )
    lam = lax.dynamic_index_in_dim(lams, owner, axis=0, keepdims=False)
    lam = jnp.broadcast_to(lam[:, :, None], (2, rows, lanes))

    def shifted(value, offset):
        pairs = [(i, i + offset) for i in range(blocks) if 0 <= i + offset < blocks]
        return lax.ppermute(value, "blocks", pairs)

    left = shifted(to_right, 1)
    right = shifted(to_left, -1)
    (back,) = make_sweeps(own, depth, rows, lanes, ny)(left, spec, right, kap, lam)
    back = lax.all_to_all(back, ROW, split_axis=0, concat_axis=0, tiled=True)
    (near,) = make_backward(total, own, lanes)(second_mat, back)
    near = lax.all_to_all(
        near.reshape(own, -1, lanes), TM[1:], split_axis=0, concat_axis=0, tiled=True
    )
    (far,) = make_turn(blocks, own, lanes)(near.reshape(-1, lanes))
    times = lax.all_to_all(
        far.reshape(blocks, 3 * own + 1, 1, lanes), "blocks", split_axis=0, concat_axis=0, tiled=True
    )
    new_iterate, new_residual = make_exit(nz, ny, nx, blocks, own)(times.reshape(-1, lanes), u)
    return (new_iterate[None], new_residual[None])


def solution(mesh):
    split = Mesh(
        mesh.devices.reshape(mesh.shape["groups"], 16, 2, 4, mesh.shape["space"]),
        ("groups", "blocks", "pair", "tm_1", "space"),
    )
    placed = (
        P(GROUPS_TM, "space", None, None),
        P(GROUPS_TM, "space", None, None),
        P(("groups", "space"), None, None),
    )
    return jax.shard_map(
        on_device,
        mesh=split,
        in_specs=placed,
        out_specs=(P(GROUPS_TM, "space", None, None), P(GROUPS_TM, "space", None, None)),
        check_vma=False,
    )
```

```python
import math

import jax
import jax.numpy as jnp
import numpy as np
from jax import lax
from jax.experimental import pallas as pl
from jax.experimental.pallas import tpu as pltpu
from jax.sharding import Mesh
from jax.sharding import PartitionSpec as P


SWEEPS = 6
TM = ("blocks", "pair", "tm_1")
ROW = ("pair", "tm_1", "space")
GROUPS_TM = ("groups", "blocks", "pair", "tm_1")
HIGH = lax.Precision.HIGHEST

frac_order = 0.3
step_length = 0.01
gamma_factor = 0.9086387328532904


def history_weights(count):
    k = np.arange(count + 1, dtype=np.float64) ** (1.0 - frac_order)
    b = k[1:] - k[:-1]
    d = np.concatenate([[1.0], b[1:] - b[:-1]])
    return d / (step_length**frac_order * gamma_factor)


def tables(total, owners, own):
    half = total // 2
    here = half // owners
    n = np.arange(total)
    d = history_weights(total)
    lag = n[:, None] - n[None, :]
    hist = np.where(lag >= 0, d[np.maximum(lag, 0)], 0.0)
    first = np.where(n < half, d, 0.0)
    angle = 2.0 * math.pi * ((n[:, None] * n[None, :]) % total) / total
    lam = (first[None, :] * np.exp(-1j * angle)).sum(1)
    fwd = np.zeros((owners, 2, here, total))
    inv = np.zeros((total, owners, 2, here))
    lams = np.zeros((owners, 2, 2, here))
    for q in range(owners):
        for j in range(here):
            k = q * here + j
            if k == 0:
                fwd[q, 0, j] = 1.0
                fwd[q, 1, j] = np.cos(angle[half])
                inv[:, q, 0, j] = 1.0 / total
                inv[:, q, 1, j] = np.cos(angle[half]) / total
                lams[q, 0, :, j] = lam[0].real, lam[half].real
            else:
                fwd[q, 0, j] = np.cos(angle[k])
                fwd[q, 1, j] = -np.sin(angle[k])
                inv[:, q, 0, j] = 2.0 * np.cos(angle[k]) / total
                inv[:, q, 1, j] = -2.0 * np.sin(angle[k]) / total
                lams[q, 0, :, j] = lam[k].real
                lams[q, 1, :, j] = lam[k].imag
    fwd = fwd.reshape(total, total)
    first_mat = np.zeros((2 * total, total, 2))
    spectra = first_mat.reshape(owners, 2, 2 * here, total, 2)
    spectra[:, 0, :, :, 0] = (-fwd @ hist).reshape(owners, 2 * here, total)
    spectra[:, 0, :, :, 1] = fwd.reshape(owners, 2 * here, total)
    spectra[:, 1, :, :, 0] = fwd.reshape(owners, 2 * here, total)
    flat = inv.reshape(total, total)
    second_mat = np.stack([hist @ flat, flat]).reshape(2, total // own, own, total)
    second_mat = second_mat.transpose(0, 2, 1, 3)
    f32 = np.float32
    return (
        first_mat.reshape(2 * total, 2 * total).astype(f32),
        second_mat.reshape(2 * total, total).astype(f32),
        lams.reshape(owners, 2, 2 * here).astype(f32),
    )


def local_call(kernel, outs, inputs, scratch=(), keep_in=True, keep_out=True):
    vmem = pl.BlockSpec(memory_space=pltpu.VMEM)
    made = pltpu.VMEM if keep_out else jax.ShapeDtypeStruct
    call = pl.pallas_call(
        kernel,
        out_shape=[made(shape, jnp.float32) for shape in outs],
        in_specs=[vmem] * inputs,
        out_specs=[vmem] * len(outs),
        scratch_shapes=list(scratch),
    )

    def placed(*args):
        if keep_in:
            args = [pltpu.with_memory_space_constraint(a, pltpu.VMEM) for a in args]
        return call(*args)

    return placed


def iota(shape, dim):
    return lax.broadcasted_iota(jnp.int32, shape, dim)


def make_entry(nz, ny, nx):
    lanes = nz * ny

    def kernel(u, f, kappa, out, s):
        row, lane = iota((ny, nx), 0), iota((ny, nx), 1)
        for z in range(nz):
            v = u[z]
            near = jnp.where(row == 0, 0.0, pltpu.roll(v, 1, 0))
            near = near + jnp.where(row == ny - 1, 0.0, pltpu.roll(v, ny - 1, 0))
            near = near + jnp.where(lane == 0, 0.0, pltpu.roll(v, 1, 1))
            near = near + jnp.where(lane == nx - 1, 0.0, pltpu.roll(v, nx - 1, 1))
            if z > 0:
                near = near + u[z - 1]
            if z < nz - 1:
                near = near + u[z + 1]
            s[z] = f[z] - kappa[z] * (6.0 * v - near)
        out[pl.ds(0, nx, stride=2), :] = u[...].reshape(lanes, nx).T
        out[pl.ds(1, nx, stride=2), :] = s[...].reshape(lanes, nx).T

    scratch = [pltpu.VMEM((nz, ny, nx), jnp.float32)]
    return local_call(kernel, [(2 * nx, lanes)], 3, scratch, keep_in=False)


def make_forward(total, owners, lanes, ny):
    rows = total // owners

    def kernel(mat, cells, info, out, both):
        both[...] = jnp.dot(
            mat[...], cells[...], precision=HIGH, preferred_element_type=jnp.float32
        )
        lane = iota((owners, lanes), 1)
        lower = info[3:4, :]
        edge = jnp.zeros((owners, lanes), jnp.float32)
        for j in range(rows):
            x = both[pl.ds(rows + j, owners, stride=2 * rows), :]
            at = ny * (rows - 1 - j)
            moved = lower * pltpu.roll(x, (at + ny) % lanes, 1) + (1.0 - lower) * (
                pltpu.roll(x, at, 1) if at else x
            )
            edge = jnp.where((lane >= at) & (lane < at + ny), moved, edge)
        for q in range(owners):
            out[12 * q : 12 * q + rows, :] = both[2 * rows * q : 2 * rows * q + rows, :]
        out[pl.ds(rows, owners, stride=12), :] = edge
        for m in range(3):
            row = jnp.broadcast_to(info[m : m + 1, :], (owners, lanes))
            out[pl.ds(rows + 1 + m, owners, stride=12), :] = row

    scratch = [pltpu.VMEM((2 * total, lanes), jnp.float32)]
    return local_call(kernel, [(12 * owners, lanes)], 3, scratch)


def make_border(own, depth, rows, lanes, ny):
    def kernel(spec, out, to_right, to_left, kap):
        lane = iota((rows, lanes), 1)
        first, last = lane < ny, lane >= lanes - ny
        for c in range(own):
            for h in range(2):
                for m in range(3):
                    if c + own * m < own + 2 * depth:
                        at = 2 * (c + own * m) + h
                        line = 12 * (2 * c + h) + rows + 1 + m
                        kap[at : at + 1, :] = spec[line : line + 1, :]
        for c in range(own):
            for h in range(2):
                at = 2 * (depth + c) + h
                k = jnp.broadcast_to(kap[at : at + 1, :], (rows, lanes))
                line = 12 * (2 * c + 1 - h) + rows
                edge = jnp.broadcast_to(spec[line : line + 1, :], (rows, lanes))
                other = pltpu.roll(edge, ny if h else 0, 1, stride=ny, stride_axis=0)
                line = 12 * (2 * c + h)
                value = spec[line : line + rows, :] + jnp.where(first if h else last, k * other, 0.0)
                out[c, h] = value
                if c >= own - depth:
                    to_right[c - (own - depth), h] = value
                if c < depth:
                    to_left[c, h] = value

    shapes = [(count, 2, rows, lanes) for count in (own, depth, depth)]
    return local_call(kernel, shapes + [(2 * (own + 2 * depth), lanes)], 1)


def make_backward(total, own, lanes):
    blocks = total // own
    pad = 3 * blocks + 8

    def kernel(mat, back, out):
        def fields(k):
            return jnp.concatenate([back[:, 3 * h + k].reshape(total, lanes) for h in range(2)], 1)

        def product(m, x):
            return jnp.dot(m, x, precision=HIGH, preferred_element_type=jnp.float32)

        first = product(mat[...], fields(0))
        rest = product(mat[total:, :], jnp.concatenate([fields(1), fields(2)], axis=1))
        correction = first[total:]
        image = first[:total] + rest[:, : 2 * lanes]
        residual = rest[:, 2 * lanes :]
        ri, ii = residual * image, image * image
        for c in range(own):
            for k, field in enumerate((correction, image, residual)):
                at = pad * c + blocks * k
                out[at : at + blocks, :] = field[blocks * c : blocks * (c + 1), :lanes]
        ri = jnp.sum(ri[:, :lanes] + ri[:, lanes:], axis=0, keepdims=True)
        ii = jnp.sum(ii[:, :lanes] + ii[:, lanes:], axis=0, keepdims=True)
        low = iota((1, lanes), 1) < lanes // 2
        sums = jnp.where(low, ri + pltpu.roll(ri, lanes // 2, 1), ii + pltpu.roll(ii, lanes // 2, 1))
        for c in range(own):
            out[pad * c + 3 * blocks : pad * (c + 1), :] = jnp.broadcast_to(sums, (8, lanes))

    return local_call(kernel, [(own * pad, lanes)], 2)


def make_turn(blocks, own, lanes):
    pad, rows = 3 * blocks + 8, 3 * own + 1

    def kernel(near, out):
        sums = 0.0
        for c in range(own):
            for k in range(3):
                at = pad * c + blocks * k
                out[pl.ds(own * k + c, blocks, stride=rows), :] = near[at : at + blocks, :]
            sums = sums + near[pad * c + 3 * blocks : pad * c + 3 * blocks + 1, :]
        out[pl.ds(3 * own, blocks, stride=rows), :] = jnp.broadcast_to(sums, (blocks, lanes))

    return local_call(kernel, [(blocks * rows, lanes)], 1)


def make_exit(nz, ny, nx, blocks, own):
    lanes = nz * ny
    rows = 3 * own + 1

    def kernel(times, u, new_u, new_r):
        low = iota((1, lanes), 1) < lanes // 2
        row = jnp.sum(times[pl.ds(3 * own, blocks, stride=rows), :], axis=0, keepdims=True)
        ri = jnp.sum(jnp.where(low, row, 0.0), axis=1, keepdims=True)
        ii = jnp.sum(jnp.where(low, 0.0, row), axis=1, keepdims=True)
        step = (ri / ii).reshape(1, 1, 1)

        def slab(k):
            parts = [times[rows * b + own * k : rows * b + own * (k + 1), :] for b in range(blocks)]
            return jnp.concatenate(parts, axis=0).T.reshape(nz, ny, nx)

        new_u[...] = u[...] + step * slab(0)
        new_r[...] = slab(2) - step * slab(1)

    return local_call(kernel, [(nz, ny, nx)] * 2, 2, keep_out=False)


def make_sweeps(own, depth, rows, lanes, ny):
    cols = own + 2 * depth
    shape = (rows, lanes)

    def kernel(left, mid, right, kap, lam, out, start, same, cross, ping, pong):
        flat = [(ref, c) for ref in (left, mid, right) for c in range(ref.shape[0])]
        lane = iota(shape, 1)
        y = lane % ny
        y_first, y_last = y == 0, y == ny - 1
        z_first, z_last = lane < ny, lane >= lanes - ny
        sign = jnp.where(iota(shape, 0) < rows // 2, -1.0, 1.0)
        lam_r, lam_i = lam[0], lam[1]
        lam_ii = lam_i * lam_i

        def swap(v):
            return pltpu.roll(v, rows // 2, 0)

        for c in range(cols):
            ref, at = flat[c]
            for h in range(2):
                k = jnp.broadcast_to(kap[2 * c + h : 2 * c + h + 1, :], shape)
                diag = lam_r + 6.0 * k
                over = 1.0 / (diag * diag + lam_ii)
                g = diag * over
                g_cross = sign * (-lam_i * over)
                spec = ref[at, h]
                first = g * spec + g_cross * swap(spec)
                start[c, h] = first
                ping[c, h] = first
                same[c, h] = g * k
                cross[c, h] = g_cross * k

        def around(buf, c):
            a, b = buf[c, 0], buf[c, 1]
            down_a, down_b = pltpu.roll(a, ny, 1), pltpu.roll(b, ny, 1)
            up_a, up_b = pltpu.roll(a, lanes - ny, 1), pltpu.roll(b, lanes - ny, 1)

            def along_y(v):
                return jnp.where(y_first, 0.0, pltpu.roll(v, 1, 1)) + jnp.where(
                    y_last, 0.0, pltpu.roll(v, lanes - 1, 1)
                )

            na = jnp.where(z_first, 0.0, down_a) + jnp.where(z_last, up_b, up_a) + along_y(a)
            nb = jnp.where(z_first, down_a, down_b) + jnp.where(z_last, 0.0, up_b) + along_y(b)
            return (
                na + buf[c - 1, 0] + buf[c + 1, 0],
                nb + buf[c - 1, 1] + buf[c + 1, 1],
            )

        now, then = ping, pong
        for sweep in range(1, SWEEPS):
            for c in range(sweep, cols - sweep):
                near = around(now, c)
                for h in range(2):
                    n = near[h]
                    then[c, h] = start[c, h] + (same[c, h] * n + cross[c, h] * swap(n))
            now, then = then, now
        for c in range(depth, depth + own):
            near = around(now, c)
            for h in range(2):
                sol = now[c, h]
                k = jnp.broadcast_to(kap[2 * c + h : 2 * c + h + 1, :], shape)
                stiff = k * (6.0 * sol - near[h])
                for core in range(2):
                    row, at = 2 * (c - depth) + core, 0 if core == h else 3
                    out[row, at] = sol
                    out[row, at + 1] = stiff
                    out[row, at + 2] = mid[c - depth, h]

    field = pltpu.VMEM((cols, 2, rows, lanes), jnp.float32)
    return local_call(kernel, [(2 * own, 6, rows, lanes)], 5, [field] * 5)


def on_device(iterate, source, diffusivity):
    _, nz, ny, nx = iterate.shape
    lanes = nz * ny
    blocks, pair = lax.axis_size("blocks"), lax.axis_size("pair")
    own = pair * lax.axis_size("tm_1")
    cores = lax.axis_size("space")
    total = blocks * own
    owners = own * cores
    rows = total // owners
    depth = SWEEPS
    first_mat, second_mat, lams = tables(total, owners, own)
    core = lax.axis_index("space")
    block = lax.axis_index("blocks")

    u, f = iterate[0], source[0]
    (send,) = make_entry(nz, ny, nx)(u, f, diffusivity)
    start = block * own + lax.axis_index(TM[1:])
    owner = lax.axis_index(ROW)
    lower = jnp.where(core == 0, 1.0, 0.0)
    send, start, owner, lower = lax.optimization_barrier((send, start, owner, lower))
    cells = lax.all_to_all(
        send.reshape(total, 2, lanes), TM, split_axis=0, concat_axis=0, tiled=True
    ).reshape(2 * total, lanes)

    cells, kappa, start, lower = lax.optimization_barrier((cells, diffusivity, start, lower))
    columns = jnp.pad(kappa.reshape(lanes, nx).T, ((depth, 2 * own), (0, 0)))
    columns = lax.dynamic_slice_in_dim(columns, start, 2 * own + 1, axis=0)
    lower = jnp.broadcast_to(lower, (1, lanes))
    info = jnp.concatenate([columns[0:1], columns[own : own + 1], columns[2 * own :], lower], axis=0)
    (spec,) = make_forward(total, owners, lanes, ny)(first_mat, cells, info)
    spec = lax.all_to_all(
        spec.reshape(owners, 12, 1, lanes), ROW, split_axis=0, concat_axis=0, tiled=True
    )
    spec, to_right, to_left, kap = make_border(own, depth, rows, lanes, ny)(spec.reshape(-1, lanes))
    to_right, to_left, lams, owner = lax.optimization_barrier(
        (to_right, to_left, jnp.asarray(lams), owner)
    )
    lam = lax.dynamic_index_in_dim(lams, owner, axis=0, keepdims=False)
    lam = jnp.broadcast_to(lam[:, :, None], (2, rows, lanes))

    def shifted(value, offset):
        pairs = [(i, i + offset) for i in range(blocks) if 0 <= i + offset < blocks]
        return lax.ppermute(value, "blocks", pairs)

    right = shifted(to_left, -1)
    left = shifted(to_right, 1)
    (back,) = make_sweeps(own, depth, rows, lanes, ny)(left, spec, right, kap, lam)
    back = lax.all_to_all(back, ROW, split_axis=0, concat_axis=0, tiled=True)
    (near,) = make_backward(total, own, lanes)(second_mat, back)
    near = lax.all_to_all(
        near.reshape(own, -1, lanes), TM[1:], split_axis=0, concat_axis=0, tiled=True
    )
    (far,) = make_turn(blocks, own, lanes)(near.reshape(-1, lanes))
    times = lax.all_to_all(
        far.reshape(blocks, 3 * own + 1, 1, lanes), "blocks", split_axis=0, concat_axis=0, tiled=True
    )
    new_iterate, new_residual = make_exit(nz, ny, nx, blocks, own)(times.reshape(-1, lanes), u)
    return (new_iterate[None], new_residual[None])


def solution(mesh):
    split = Mesh(
        mesh.devices.reshape(mesh.shape["groups"], 16, 2, 4, mesh.shape["space"]),
        ("groups", "blocks", "pair", "tm_1", "space"),
    )
    placed = (
        P(GROUPS_TM, "space", None, None),
        P(GROUPS_TM, "space", None, None),
        P(("groups", "space"), None, None),
    )
    return jax.shard_map(
        on_device,
        mesh=split,
        in_specs=placed,
        out_specs=(P(GROUPS_TM, "space", None, None), P(GROUPS_TM, "space", None, None)),
        check_vma=False,
    )
```

```python
import math

import jax
import jax.numpy as jnp
import numpy as np
from jax import lax
from jax.experimental import pallas as pl
from jax.experimental.pallas import tpu as pltpu
from jax.sharding import Mesh
from jax.sharding import PartitionSpec as P

SWEEPS = 6
TM = ("blocks", "pair", "tm_1")
ROW = ("pair", "tm_1", "space")
GROUPS_TM = ("groups", "blocks", "pair", "tm_1")
HIGH = lax.Precision.HIGHEST

frac_order = 0.3
step_length = 0.01
gamma_factor = 0.9086387328532904


def history_weights(count):
    k = np.arange(count + 1, dtype=np.float64) ** (1.0 - frac_order)
    b = k[1:] - k[:-1]
    d = np.concatenate([[1.0], b[1:] - b[:-1]])
    return d / (step_length**frac_order * gamma_factor)


def tables(total, owners, own):
    half = total // 2
    here = half // owners
    n = np.arange(total)
    d = history_weights(total)
    lag = n[:, None] - n[None, :]
    hist = np.where(lag >= 0, d[np.maximum(lag, 0)], 0.0)
    first = np.where(n < half, d, 0.0)
    angle = 2.0 * math.pi * ((n[:, None] * n[None, :]) % total) / total
    lam = (first[None, :] * np.exp(-1j * angle)).sum(1)
    fwd = np.zeros((owners, 2, here, total))
    inv = np.zeros((total, owners, 2, here))
    lams = np.zeros((owners, 2, 2, here))
    for q in range(owners):
        for j in range(here):
            k = q * here + j
            if k == 0:
                fwd[q, 0, j] = 1.0
                fwd[q, 1, j] = np.cos(angle[half])
                inv[:, q, 0, j] = 1.0 / total
                inv[:, q, 1, j] = np.cos(angle[half]) / total
                lams[q, 0, :, j] = lam[0].real, lam[half].real
            else:
                fwd[q, 0, j] = np.cos(angle[k])
                fwd[q, 1, j] = -np.sin(angle[k])
                inv[:, q, 0, j] = 2.0 * np.cos(angle[k]) / total
                inv[:, q, 1, j] = -2.0 * np.sin(angle[k]) / total
                lams[q, 0, :, j] = lam[k].real
                lams[q, 1, :, j] = lam[k].imag
    fwd = fwd.reshape(total, total)
    first_mat = np.zeros((2 * total, total, 2))
    spectra = first_mat.reshape(owners, 2, 2 * here, total, 2)
    spectra[:, 0, :, :, 0] = (-fwd @ hist).reshape(owners, 2 * here, total)
    spectra[:, 0, :, :, 1] = fwd.reshape(owners, 2 * here, total)
    spectra[:, 1, :, :, 0] = fwd.reshape(owners, 2 * here, total)
    flat = inv.reshape(total, total)
    second_mat = np.stack([hist @ flat, flat]).reshape(2, total // own, own, total)
    second_mat = second_mat.transpose(0, 2, 1, 3)
    f32 = np.float32
    return (
        first_mat.reshape(2 * total, 2 * total).astype(f32),
        second_mat.reshape(2 * total, total).astype(f32),
        lams.reshape(owners, 2, 2 * here).astype(f32),
    )


def local_call(kernel, name, outs, inputs, scratch=(), keep_in=True, keep_out=True):
    vmem = pl.BlockSpec(memory_space=pltpu.VMEM)
    made = pltpu.VMEM if keep_out else jax.ShapeDtypeStruct
    call = pl.pallas_call(
        kernel,
        out_shape=[made(shape, jnp.float32) for shape in outs],
        in_specs=[vmem] * inputs,
        out_specs=[vmem] * len(outs),
        scratch_shapes=list(scratch),
        name=name,
    )

    def placed(*args):
        if keep_in:
            args = [pltpu.with_memory_space_constraint(a, pltpu.VMEM) for a in args]
        return call(*args)

    return placed


def iota(shape, dim):
    return lax.broadcasted_iota(jnp.int32, shape, dim)


def make_entry(nz, ny, nx):
    lanes = nz * ny

    def kernel(u, f, kappa, out, s):
        row, lane = iota((ny, nx), 0), iota((ny, nx), 1)
        for z in range(nz):
            v = u[z]
            near = jnp.where(row == 0, 0.0, pltpu.roll(v, 1, 0))
            near = near + jnp.where(row == ny - 1, 0.0, pltpu.roll(v, ny - 1, 0))
            near = near + jnp.where(lane == 0, 0.0, pltpu.roll(v, 1, 1))
            near = near + jnp.where(lane == nx - 1, 0.0, pltpu.roll(v, nx - 1, 1))
            if z > 0:
                near = near + u[z - 1]
            if z < nz - 1:
                near = near + u[z + 1]
            s[z] = f[z] - kappa[z] * (6.0 * v - near)
        out[pl.ds(0, nx, stride=2), :] = u[...].reshape(lanes, nx).T
        out[pl.ds(1, nx, stride=2), :] = s[...].reshape(lanes, nx).T

    scratch = [pltpu.VMEM((nz, ny, nx), jnp.float32)]
    return local_call(kernel, "entry", [(2 * nx, lanes)], 3, scratch, keep_in=False)


def make_forward(total, owners, lanes, ny):
    rows = total // owners

    def kernel(mat, cells, info, out, both):
        both[...] = jnp.dot(
            mat[...], cells[...], precision=HIGH, preferred_element_type=jnp.float32
        )
        lane = iota((owners, lanes), 1)
        lower = info[3:4, :]
        edge = jnp.zeros((owners, lanes), jnp.float32)
        for j in range(rows):
            x = both[pl.ds(rows + j, owners, stride=2 * rows), :]
            at = ny * (rows - 1 - j)
            moved = lower * pltpu.roll(x, (at + ny) % lanes, 1) + (1.0 - lower) * (
                pltpu.roll(x, at, 1) if at else x
            )
            edge = jnp.where((lane >= at) & (lane < at + ny), moved, edge)
        for q in range(owners):
            out[16 * q : 16 * q + rows, :] = both[2 * rows * q : 2 * rows * q + rows, :]
        out[pl.ds(rows, owners, stride=16), :] = edge
        for m in range(3):
            row = jnp.broadcast_to(info[m : m + 1, :], (owners, lanes))
            out[pl.ds(rows + 1 + m, owners, stride=16), :] = row
        for m in range(rows + 4, 16):
            out[pl.ds(m, owners, stride=16), :] = edge

    scratch = [pltpu.VMEM((2 * total, lanes), jnp.float32)]
    return local_call(kernel, "forward", [(16 * owners, lanes)], 3, scratch)


def make_border(own, depth, rows, lanes, ny):
    def kernel(spec, out, to_right, to_left, kap):
        lane = iota((rows, lanes), 1)
        first, last = lane < ny, lane >= lanes - ny
        for c in range(own):
            for h in range(2):
                for m in range(3):
                    if c + own * m < own + 2 * depth:
                        at = 2 * (c + own * m) + h
                        line = 16 * (2 * c + h) + rows + 1 + m
                        kap[at : at + 1, :] = spec[line : line + 1, :]
        for c in range(own):
            for h in range(2):
                at = 2 * (depth + c) + h
                k = jnp.broadcast_to(kap[at : at + 1, :], (rows, lanes))
                line = 16 * (2 * c + 1 - h) + rows
                edge = jnp.broadcast_to(spec[line : line + 1, :], (rows, lanes))
                other = pltpu.roll(edge, ny if h else 0, 1, stride=ny, stride_axis=0)
                line = 16 * (2 * c + h)
                value = spec[line : line + rows, :] + jnp.where(first if h else last, k * other, 0.0)
                out[c, h] = value
                if c >= own - depth:
                    to_right[c - (own - depth), h] = value
                if c < depth:
                    to_left[c, h] = value

    shapes = [(count, 2, rows, lanes) for count in (own, depth, depth)]
    return local_call(kernel, "border", shapes + [(2 * (own + 2 * depth), lanes)], 1)


def make_backward(total, own, lanes):
    blocks = total // own
    pad = 3 * blocks + 8

    def kernel(mat, back, out):
        def fields(k):
            return jnp.concatenate([back[:, 3 * h + k].reshape(total, lanes) for h in range(2)], 1)

        def product(m, x):
            return jnp.dot(m, x, precision=HIGH, preferred_element_type=jnp.float32)

        first = product(mat[...], fields(0))
        rest = product(mat[total:, :], jnp.concatenate([fields(1), fields(2)], axis=1))
        correction = first[total:]
        image = first[:total] + rest[:, : 2 * lanes]
        residual = rest[:, 2 * lanes :]
        ri, ii = residual * image, image * image
        for c in range(own):
            for k, field in enumerate((correction, image, residual)):
                at = pad * c + blocks * k
                out[at : at + blocks, :] = field[blocks * c : blocks * (c + 1), :lanes]
        ri = jnp.sum(ri[:, :lanes] + ri[:, lanes:], axis=0, keepdims=True)
        ii = jnp.sum(ii[:, :lanes] + ii[:, lanes:], axis=0, keepdims=True)
        low = iota((1, lanes), 1) < lanes // 2
        sums = jnp.where(low, ri + pltpu.roll(ri, lanes // 2, 1), ii + pltpu.roll(ii, lanes // 2, 1))
        for c in range(own):
            out[pad * c + 3 * blocks : pad * (c + 1), :] = jnp.broadcast_to(sums, (8, lanes))

    return local_call(kernel, "backward", [(own * pad, lanes)], 2)


def make_turn(blocks, own, lanes):
    pad, rows = 3 * blocks + 8, 3 * own + 1

    def kernel(near, out):
        sums = 0.0
        for c in range(own):
            for k in range(3):
                at = pad * c + blocks * k
                out[pl.ds(own * k + c, blocks, stride=rows), :] = near[at : at + blocks, :]
            sums = sums + near[pad * c + 3 * blocks : pad * c + 3 * blocks + 1, :]
        out[pl.ds(3 * own, blocks, stride=rows), :] = jnp.broadcast_to(sums, (blocks, lanes))

    return local_call(kernel, "turn", [(blocks * rows, lanes)], 1)


def make_exit(nz, ny, nx, blocks, own):
    lanes = nz * ny
    rows = 3 * own + 1

    def kernel(times, u, new_u, new_r):
        low = iota((1, lanes), 1) < lanes // 2
        row = jnp.sum(times[pl.ds(3 * own, blocks, stride=rows), :], axis=0, keepdims=True)
        ri = jnp.sum(jnp.where(low, row, 0.0), axis=1, keepdims=True)
        ii = jnp.sum(jnp.where(low, 0.0, row), axis=1, keepdims=True)
        step = (ri / ii).reshape(1, 1, 1)

        def slab(k):
            parts = [times[rows * b + own * k : rows * b + own * (k + 1), :] for b in range(blocks)]
            return jnp.concatenate(parts, axis=0).T.reshape(nz, ny, nx)

        new_u[...] = u[...] + step * slab(0)
        new_r[...] = slab(2) - step * slab(1)

    return local_call(kernel, "exit", [(nz, ny, nx)] * 2, 2, keep_out=False)


def make_sweeps(own, depth, rows, lanes, ny):
    cols = own + 2 * depth
    shape = (rows, lanes)

    def kernel(left, mid, right, kap, lam, out, start, same, cross, ping, pong):
        flat = [(ref, c) for ref in (left, mid, right) for c in range(ref.shape[0])]
        lane = iota(shape, 1)
        y = lane % ny
        y_first, y_last = y == 0, y == ny - 1
        z_first, z_last = lane < ny, lane >= lanes - ny
        sign = jnp.where(iota(shape, 0) < rows // 2, -1.0, 1.0)
        lam_r, lam_i = lam[0], lam[1]
        lam_ii = lam_i * lam_i

        def swap(v):
            return pltpu.roll(v, rows // 2, 0)

        for c in range(cols):
            ref, at = flat[c]
            for h in range(2):
                k = jnp.broadcast_to(kap[2 * c + h : 2 * c + h + 1, :], shape)
                diag = lam_r + 6.0 * k
                over = 1.0 / (diag * diag + lam_ii)
                g = diag * over
                g_cross = sign * (-lam_i * over)
                spec = ref[at, h]
                first = g * spec + g_cross * swap(spec)
                start[c, h] = first
                ping[c, h] = first
                same[c, h] = g * k
                cross[c, h] = g_cross * k

        def around(buf, c):
            a, b = buf[c, 0], buf[c, 1]
            down_a, down_b = pltpu.roll(a, ny, 1), pltpu.roll(b, ny, 1)
            up_a, up_b = pltpu.roll(a, lanes - ny, 1), pltpu.roll(b, lanes - ny, 1)

            def along_y(v):
                return jnp.where(y_first, 0.0, pltpu.roll(v, 1, 1)) + jnp.where(
                    y_last, 0.0, pltpu.roll(v, lanes - 1, 1)
                )

            na = jnp.where(z_first, 0.0, down_a) + jnp.where(z_last, up_b, up_a) + along_y(a)
            nb = jnp.where(z_first, down_a, down_b) + jnp.where(z_last, 0.0, up_b) + along_y(b)
            return (
                na + buf[c - 1, 0] + buf[c + 1, 0],
                nb + buf[c - 1, 1] + buf[c + 1, 1],
            )

        now, then = ping, pong
        for sweep in range(1, SWEEPS):
            for c in range(sweep, cols - sweep):
                near = around(now, c)
                for h in range(2):
                    n = near[h]
                    then[c, h] = start[c, h] + (same[c, h] * n + cross[c, h] * swap(n))
            now, then = then, now
        for c in range(depth, depth + own):
            near = around(now, c)
            for h in range(2):
                sol = now[c, h]
                k = jnp.broadcast_to(kap[2 * c + h : 2 * c + h + 1, :], shape)
                stiff = k * (6.0 * sol - near[h])
                for core in range(2):
                    row, at = 2 * (c - depth) + core, 0 if core == h else 3
                    out[row, at] = sol
                    out[row, at + 1] = stiff
                    out[row, at + 2] = mid[c - depth, h]

    field = pltpu.VMEM((cols, 2, rows, lanes), jnp.float32)
    return local_call(kernel, "sweeps", [(2 * own, 6, rows, lanes)], 5, [field] * 5)


def on_device(iterate, source, diffusivity):
    _, nz, ny, nx = iterate.shape
    lanes = nz * ny
    blocks, pair = lax.axis_size("blocks"), lax.axis_size("pair")
    own = pair * lax.axis_size("tm_1")
    cores = lax.axis_size("space")
    total = blocks * own
    owners = own * cores
    rows = total // owners
    depth = SWEEPS
    first_mat, second_mat, lams = tables(total, owners, own)
    core = lax.axis_index("space")
    block = lax.axis_index("blocks")

    u, f = iterate[0], source[0]
    (send,) = make_entry(nz, ny, nx)(u, f, diffusivity)
    start = block * own + lax.axis_index(TM[1:])
    owner = lax.axis_index(ROW)
    lower = jnp.where(core == 0, 1.0, 0.0)
    send, start, owner, lower = lax.optimization_barrier((send, start, owner, lower))
    cells = lax.all_to_all(
        send.reshape(total, 2, lanes), TM, split_axis=0, concat_axis=0, tiled=True
    ).reshape(2 * total, lanes)

    cells, kappa, start, lower = lax.optimization_barrier((cells, diffusivity, start, lower))
    columns = jnp.pad(kappa.reshape(lanes, nx).T, ((depth, 2 * own), (0, 0)))
    columns = lax.dynamic_slice_in_dim(columns, start, 2 * own + 1, axis=0)
    lower = jnp.broadcast_to(lower, (1, lanes))
    info = jnp.concatenate([columns[0:1], columns[own : own + 1], columns[2 * own :], lower], axis=0)
    (spec,) = make_forward(total, owners, lanes, ny)(first_mat, cells, info)
    spec = lax.all_to_all(
        spec.reshape(owners, 16, lanes), ROW, split_axis=0, concat_axis=0, tiled=True
    )
    spec, to_right, to_left, kap = make_border(own, depth, rows, lanes, ny)(spec.reshape(-1, lanes))
    to_right, to_left, lams, owner = lax.optimization_barrier(
        (to_right, to_left, jnp.asarray(lams), owner)
    )
    lam = lax.dynamic_index_in_dim(lams, owner, axis=0, keepdims=False)
    lam = jnp.broadcast_to(lam[:, :, None], (2, rows, lanes))

    def shifted(value, offset):
        pairs = [(i, i + offset) for i in range(blocks) if 0 <= i + offset < blocks]
        return lax.ppermute(value, "blocks", pairs)

    left = shifted(to_right, 1)
    right = shifted(to_left, -1)
    (back,) = make_sweeps(own, depth, rows, lanes, ny)(left, spec, right, kap, lam)
    back = lax.all_to_all(back, ROW, split_axis=0, concat_axis=0, tiled=True)
    (near,) = make_backward(total, own, lanes)(second_mat, back)
    near = lax.all_to_all(
        near.reshape(own, -1, lanes), TM[1:], split_axis=0, concat_axis=0, tiled=True
    )
    (far,) = make_turn(blocks, own, lanes)(near.reshape(-1, lanes))
    times = lax.all_to_all(
        far.reshape(blocks, 3 * own + 1, 1, lanes), "blocks", split_axis=0, concat_axis=0, tiled=True
    )
    new_iterate, new_residual = make_exit(nz, ny, nx, blocks, own)(times.reshape(-1, lanes), u)
    return (new_iterate[None], new_residual[None])


def solution(mesh):
    split = Mesh(
        mesh.devices.reshape(mesh.shape["groups"], 16, 2, 4, mesh.shape["space"]),
        ("groups", "blocks", "pair", "tm_1", "space"),
    )
    placed = (
        P(GROUPS_TM, "space", None, None),
        P(GROUPS_TM, "space", None, None),
        P(("groups", "space"), None, None),
    )
    return jax.shard_map(
        on_device,
        mesh=split,
        in_specs=placed,
        out_specs=(P(GROUPS_TM, "space", None, None), P(GROUPS_TM, "space", None, None)),
        check_vma=False,
    )
```
